32 devices in a mesh: member: 2 (over x), gx: 16 (over z, y, core).
Axes of the slice: x: 2, y: 2, z: 4, core: 2. Of those that a mesh axis runs over, the one named last changes fastest.
Arguments:
- spectrum: float32 [36, 32, 256, 128], P(None, None, ('member', 'gx')), parts along dimension 2, may hold values from 0 to 1
- wind: float32 [2, 256, 128], P(None, ('member', 'gx')), parts along dimension 1, may hold values from -32 to 32
- land_sea: int32 [128, 128], P('gx'), may hold values 0 or 1
- band_rows: int32 [128], replicated, may hold values from 0 to 127, each once
Outputs:
- spectrum_next: float32 [36, 32, 256, 128], P(None, None, ('member', 'gx')), parts along dimension 2
- ocean_fields: float32 [4, 128, 256], P(None, 'gx', 'member'), parts along dimension 2
The draws below stay inside these ranges and needn't reach their ends.
There are 2 independent parts, one for each index of `member`. The reference program is written for one: setup_inputs(seed, part) draws one part's arguments, and reference() takes and returns one part's arrays. A program takes and returns all parts, laid end to end along the dimension named above; an argument that names none is the same for every part. Nothing has to cross between parts.
Inputs may be any that keep to these rules, and one draw needn't show every extreme that they name: band_rows names each of the 128 latitude rows exactly once.
All inputs are finite; a program needn't handle non-finite values. No bound on the sum of `land_sea` on one device may be relied on, other than what follows from the above.
Results may differ from the reference program's by a relative error of at most 0.00015.
Values sent between devices are 32-bit elements; how exact they have to be, the bound alone decides.
A program may use at most 128 MiB of HBM per device.

```python
import math
import jax
import jax.numpy as jnp
from jax import lax

DIRS = 36
FREQS = 32
LAT = 128
STEPS = 3
NLON = 128


def touch_ends(values, key, least, largest):
    index_at = [jax.random.randint(jax.random.fold_in(key, axis), (), 0, length) for axis, length in enumerate(values.shape)]
    longest = values.shape.index(max(values.shape))
    beside = index_at[:longest] + [(index_at[longest] + 1) % values.shape[longest]] + index_at[longest + 1:]
    return values.at[tuple(index_at)].set(least).at[tuple(beside)].set(largest)


def block_levels(own_key, shape, shards, least, largest):
    def one(position, shards_of):
        draws = jax.random.uniform(jax.random.fold_in(jax.random.fold_in(own_key, 6), position), (shards_of,), jnp.float32, least / len(shards), largest / len(shards))
        return jnp.repeat(jnp.exp(draws), shape[position] // shards_of).reshape((-1,) + (1,) * (len(shape) - position - 1))

    loudness = one(*shards[0])
    for cut in shards[1:]:
        loudness = loudness * one(*cut)
    return loudness


def centred(rng, dims, width, bound, cuts=(), kind=jnp.bfloat16):
    level = block_levels(rng, dims, cuts, -0.22, 0.18) if cuts else 1.0
    array = jax.random.normal(rng, dims, jnp.float32) * width * level
    return jnp.minimum(jnp.maximum(array, -bound), bound).astype(kind)


def setup_inputs(seed: int = 0, part: int = 0) -> dict:
    keys = jax.random.split(jax.random.key(seed), 5)
    part_keys = jax.random.split(jax.random.fold_in(keys[4], part), 5)
    spectrum = jnp.clip(1.0 * jax.random.uniform(part_keys[0], (DIRS, FREQS, NLON, LAT), jnp.float32) ** block_levels(part_keys[0], (DIRS, FREQS, NLON, LAT), ((2, 16),), -0.2, 0.2), 0.0, 1.0)
    wind = centred(part_keys[1], (2, NLON, LAT), 8.0, 32.0, ((1, 16),), jnp.float32)
    land_sea = touch_ends((jax.random.randint(keys[2], (NLON, LAT), 0, 4) < 3).astype(jnp.int32), jax.random.fold_in(keys[2], 1), 0, 1)
    band_rows = jax.random.permutation(keys[3], LAT).astype(jnp.int32)
    return dict(spectrum=spectrum, wind=wind, land_sea=land_sea, band_rows=band_rows)


def wave_tables(directions, frequencies):
    angles = (jnp.arange(directions, dtype=jnp.float32) + 0.5) * (2.0 * math.pi / directions)
    levels = jnp.arange(frequencies, dtype=jnp.float32)
    shrink = jnp.power(jnp.float32(1.1), -levels)
    frequency = 0.0418 / shrink
    inverse_speed = 2.0 * math.pi * frequency / 9.81
    weight = (levels + 1.0) / frequencies
    cosine_dir = jnp.cos(angles)[:, None]
    sine_dir = jnp.sin(angles)[:, None]
    courant_x = 0.45 * shrink[None, :] * cosine_dir
    courant_y = 0.45 * shrink[None, :] * sine_dir
    factor = 3.0 / math.sqrt(directions * frequencies)
    project = jnp.stack([factor * weight[None, :] * cosine_dir, factor * weight[None, :] * sine_dir])
    return (courant_x, courant_y, cosine_dir, sine_dir, inverse_speed, weight * weight, project)

def upwind(center, west_cell, east_cell, courant_x, courant_y):
    along_x = courant_x[:, :, None, None]
    along_y = courant_y[:, :, None, None]
    border = jnp.zeros_like(center[..., :1])
    south_cell = jnp.concatenate([border, center[..., :-1]], axis=3)
    north_cell = jnp.concatenate([center[..., 1:], border], axis=3)
    return center - jnp.maximum(along_x, 0.0) * (center - west_cell) + jnp.maximum(-along_x, 0.0) * (east_cell - center) - jnp.maximum(along_y, 0.0) * (center - south_cell) + jnp.maximum(-along_y, 0.0) * (north_cell - center)

def sources(advected, wind_east, wind_north, sea_mask, tables):
    cosine_dir, sine_dir, inverse_speed, weight_two = (tables[2], tables[3], tables[4], tables[5])
    advected = advected * sea_mask
    energy = lax.optimization_barrier(jnp.mean(advected, axis=(0, 1)))
    wind_ratio = (wind_east * cosine_dir[:, :, None, None] + wind_north * sine_dir[:, :, None, None]) * inverse_speed[None, :, None, None]
    growth = 0.05 * jnp.clip(wind_ratio - 1.0, 0.0, 4.0)
    damping = 0.3 * weight_two[None, :, None, None] * (energy / (0.5 + energy))
    return (advected * (1.0 + growth) / (1.0 + damping), growth * advected)

def coupling_fields(input_flux, current, project):
    stress = jnp.einsum('cij,ijxy->cxy', project, input_flux, precision=lax.Precision.HIGHEST)
    stokes = jnp.einsum('cij,ijxy->cxy', project, current, precision=lax.Precision.HIGHEST)
    return jnp.concatenate([stress, stokes], axis=0)

def reference(spectrum, wind, land_sea, band_rows):
    tables = wave_tables(spectrum.shape[0], spectrum.shape[1])
    sea_mask = land_sea.astype(jnp.float32)
    current = spectrum
    for step_index in range(STEPS):
        advected = upwind(current, jnp.roll(current, 1, axis=2), jnp.roll(current, -1, axis=2), tables[0], tables[1])
        current, input_flux = sources(advected, wind[0], wind[1], sea_mask, tables)
    fields = coupling_fields(input_flux, current, tables[6])
    ocean_fields = jnp.transpose(fields[:, :, band_rows], (0, 2, 1))
    return (current, ocean_fields)
```

```python
import functools
import math

import jax
import jax.numpy as jnp
from jax import lax
from jax.experimental import pallas as pl
from jax.experimental.pallas import tpu as pltpu
from jax.sharding import PartitionSpec as P

STEPS = 3
SUB = 8
LEFT, RIGHT = 8, 10


def kernel(n, dirs, groups, spec, wind_in, land_in, bands_in, out, recv,
           trig, freq, wind, land, bands, x_ref, w_ref, g_ref, send_e, send_w, halo_l, halo_r, wind_h, land_h,
           wind_b, mask_b, r_ref, drift_ref, e_send, e_halo, rows, sends,
           in_sem, small_sem, col_sem, ssem, rsem, a_ssem, a_rsem):
    me = lax.axis_index("gx")
    right, left = lax.rem(me + 1, n), lax.rem(me + n - 1, n)
    quarter = dirs // 4
    qbins = quarter * groups * SUB
    cells = dirs * groups * SUB
    lane = lax.broadcasted_iota(jnp.int32, (SUB, 128), 1)
    x_rows = x_ref.reshape(cells * SUB, 128)

    def in_copy(q):
        part = pl.ds(q * qbins, qbins)
        return pltpu.make_async_copy(spec.at[part], x_ref.at[part], in_sem.at[q])

    def column_copies(k):
        copies = []
        for j, (first, bins, target, to, column) in enumerate([
                (0, qbins, send_e, 0, SUB - 1 - k), (3 * qbins, qbins, send_e, qbins, SUB - 1 - k),
                (qbins, 2 * qbins, send_w, 0, k)]):
            copies.append(pltpu.make_async_copy(
                spec.at[pl.ds(first, bins), column], target.at[k, pl.ds(to, bins)], col_sem.at[k, j]))
        return copies

    tables_in = [pltpu.make_async_copy(src, dst, small_sem.at[i]) for i, (src, dst) in enumerate(
        [(wind_in, wind), (land_in, land), (bands_in, bands)])]
    columns_in = [column_copies(k) for k in range(3)]
    for copy in columns_in[0] + tables_in:
        copy.start()
    for q in (0, 3, 1, 2):
        in_copy(q).start()
    for copy in columns_in[1] + columns_in[2]:
        copy.start()

    for d in range(dirs):
        angle = (d + 0.5) * (2.0 * math.pi / dirs)
        trig[0, d] = jnp.float32(math.cos(angle))
        trig[1, d] = jnp.float32(math.sin(angle))
    freqs = groups * SUB
    for f in range(groups):
        level = (lax.broadcasted_iota(jnp.int32, (SUB, 128), 0) + f * SUB).astype(jnp.float32)
        weight = (level + 1.0) * (1.0 / freqs)
        grown = jnp.exp(level * math.log(1.1))
        freq[0, f] = 0.45 / grown
        freq[1, f] = grown * (2.0 * math.pi * 0.0418 / 9.81)
        freq[2, f] = 0.3 * weight * weight
        freq[3, f] = weight * (3.0 / math.sqrt(dirs * freqs))

    barrier = pltpu.get_barrier_semaphore()

    def greet(i, _):
        pl.semaphore_signal(barrier, inc=1, device_id={"gx": lax.rem(me + i, n)},
                            device_id_type=pl.DeviceIdType.MESH)
        return 0

    lax.fori_loop(1, n, greet, 0)

    def remote(src, dst, slot, target):
        return pltpu.make_async_remote_copy(
            src_ref=src, dst_ref=dst, send_sem=ssem.at[slot], recv_sem=rsem.at[slot],
            device_id={"gx": target}, device_id_type=pl.DeviceIdType.MESH)

    bulk_e = [remote(send_e.at[k], halo_l.at[k], k, right) for k in range(3)]
    bulk_w = [remote(send_w.at[k], halo_r.at[k], 3 + k, left) for k in range(3)]
    small = [remote(wind, wind_h.at[0], 6, right), remote(wind, wind_h.at[1], 7, left),
             remote(land, land_h.at[0], 8, right), remote(land, land_h.at[1], 9, left)]
    energy_msg = [[remote(e_send.at[s], e_halo.at[s, 0], 10 + 2 * s, right),
                   remote(e_send.at[s], e_halo.at[s, 1], 11 + 2 * s, left)] for s in range(2)]

    for copy in columns_in[0]:
        copy.wait()
    pl.semaphore_wait(barrier, n - 1)
    for copy in [bulk_e[0], bulk_w[0]]:
        copy.start()
    for copy in tables_in:
        copy.wait()

    def spread(slot, wind_tile, land_tile, column):
        for c in range(2):
            wind_b[c, slot] = jnp.broadcast_to(wind_tile[c][column:column + 1], (SUB, 128))
        mask_b[slot] = jnp.broadcast_to(
            land_tile[column:column + 1].astype(jnp.float32), (SUB, 128))

    own_wind = [wind[0], wind[1]]
    own_land = land[...]
    for x in range(SUB):
        spread(x, own_wind, own_land, x)

    for copy in small:
        copy.start()
    for copy in columns_in[1] + columns_in[2]:
        copy.wait()
    for copy in [bulk_e[1], bulk_w[1]]:
        copy.start()
    for q in (0, 3, 1, 2):
        in_copy(q).wait()

    def scalars(d):
        return trig[0, d], trig[1, d]

    halves = [(0, 2 * quarter, True), (quarter, 0, False)]

    def coefficients(cosine, sine, f, east, turn):
        k = freq[0, f]
        along_x = k * (cosine if east else -cosine)
        along_y = k * jnp.abs(sine)
        centre = 1.0 - along_x - along_y
        return centre, along_x, jnp.where(lane == 127 * turn, 0.0, along_y)

    def shifted(value, turn):
        return pltpu.roll(value, 1 + 126 * turn, 1)

    def growth_of(cosine, sine, f, slot):
        ratio = (wind_b[0, slot] * cosine + wind_b[1, slot] * sine) * freq[1, f]
        return 0.05 * jnp.minimum(jnp.maximum(ratio - 1.0, 0.0), 4.0)

    zero = jnp.zeros((SUB, 128), jnp.float32)

    def main(step, sums):
        for d0, skip, east in halves:
            def body(i, sums, d0=d0, skip=skip, east=east):
                turn = i // quarter
                d = d0 + i + skip * turn
                cosine, sine = scalars(d)
                sums = list(sums)
                if step == 0:
                    speed = [wind_b[0, x] * cosine + wind_b[1, x] * sine for x in range(SUB)]
                for f in range(groups):
                    centre, along_x, along_y = coefficients(cosine, sine, f, east, turn)
                    before = None
                    for x in (range(SUB) if east else range(SUB - 1, -1, -1)):
                        at = (d * groups + f) * SUB + x
                        if step == 0:
                            value = x_rows[pl.ds((d * groups + f) * SUB * SUB + x, SUB, stride=SUB), :]
                            g_ref[at] = 0.05 * jnp.minimum(
                                jnp.maximum(speed[x] * freq[1, f] - 1.0, 0.0), 4.0)
                        else:
                            value = w_ref[at] * (1.0 + g_ref[at]) * r_ref[x, f]
                        new = centre * value + along_y * shifted(value, turn)
                        if before is not None:
                            new = new + along_x * before
                        before = value
                        w_ref[at] = new
                        sums[x] = sums[x] + new
                return tuple(sums)

            sums = lax.fori_loop(0, 2 * quarter, body, tuple(sums), unroll=2)
        return sums

    def fix(step, sums):
        first, last = sums[0], sums[SUB - 1]
        for d0, skip, east in halves:
            halo = halo_l if east else halo_r
            slot = LEFT if east else RIGHT
            edge = 0 if east else SUB - 1

            def body(i, total, d0=d0, skip=skip, east=east, halo=halo, slot=slot, edge=edge):
                turn = i // quarter
                d = d0 + i + skip * turn
                cosine, sine = scalars(d)
                for f in range(groups):
                    centre, along_x, along_y = coefficients(cosine, sine, f, east, turn)
                    at = i * groups + f

                    def advance(value, upwind, depth, s):
                        moved = centre * value + along_x * upwind + along_y * shifted(value, turn)
                        growth = growth_of(cosine, sine, f, slot + depth)
                        return moved * (1.0 + growth) * r_ref[slot + depth + 4 * (s if depth == 0 else 0), f]

                    if step == 0:
                        flow = halo[0, pl.ds(at * SUB, SUB), :]
                    elif step == 1:
                        flow = advance(halo[0, pl.ds(at * SUB, SUB), :], halo[1, pl.ds(at * SUB, SUB), :], 0, 0)
                        halo[0, pl.ds(at * SUB, SUB), :] = flow
                    else:
                        far = advance(halo[1, pl.ds(at * SUB, SUB), :], halo[2, pl.ds(at * SUB, SUB), :], 1, 0)
                        flow = advance(halo[0, pl.ds(at * SUB, SUB), :], far, 0, 1)
                    extra = along_x * flow
                    cell = (d * groups + f) * SUB + edge
                    w_ref[cell] = w_ref[cell] + extra
                    total = total + extra
                return total

            if east:
                first = lax.fori_loop(0, 2 * quarter, body, first, unroll=3)
            else:
                last = lax.fori_loop(0, 2 * quarter, body, last, unroll=3)
        return (first,) + tuple(sums[1:-1]) + (last,)

    def energy_tile(sums):
        return jnp.concatenate(
            [jnp.sum(s * mask_b[x], axis=0, keepdims=True) for x, s in enumerate(sums)],
            axis=0) * (1.0 / cells)

    def factor(tile, column, mask_slot, slot):
        ratio = jnp.broadcast_to(tile[column:column + 1], (SUB, 128))
        for f in range(groups):
            r_ref[slot, f] = mask_b[mask_slot] / (1.0 + freq[2, f] * ratio)

    def own_factors(tile):
        ratio = tile / (0.5 + tile)
        for x in range(SUB):
            factor(ratio, x, x, x)

    sums = main(0, (zero,) * SUB)
    for copy in small:
        copy.wait()
    for side in range(2):
        tiles = [wind_h[side, 0], wind_h[side, 1]]
        land_tile = land_h[side]
        for depth in range(2):
            spread((LEFT if side == 0 else RIGHT) + depth, tiles, land_tile,
                   SUB - 1 - depth if side == 0 else depth)
    bulk_e[0].wait()
    bulk_w[0].wait()
    sums = fix(0, sums)
    for step in (1, 2):
        tile = energy_tile(sums)
        e_send[step - 1] = tile
        own_factors(tile)
        for copy in energy_msg[step - 1]:
            copy.start()
        if step == 1:
            bulk_e[2].start()
            bulk_w[2].start()
        sums = main(step, (zero,) * SUB)
        bulk_e[step].wait()
        bulk_w[step].wait()
        for copy in energy_msg[step - 1]:
            copy.wait()
        for side in range(2):
            seen = e_halo[step - 1, side]
            ratio = seen / (0.5 + seen)
            base = LEFT if side == 0 else RIGHT
            for depth in range(3 - step):
                factor(ratio, SUB - 1 - depth if side == 0 else depth, base + depth,
                       base + depth + 4 * (step - 1))
        sums = fix(step, sums)

    own_factors(energy_tile(sums))

    def gather(d, carry):
        cosine, sine = scalars(d)
        carry = list(carry)
        for x in range(SUB):
            flux, drift = zero, zero
            for f in range(groups):
                at = (d * groups + f) * SUB + x
                moved = w_ref[at]
                flow = g_ref[at] * moved
                flux = flux + freq[3, f] * flow
                drift = drift + drift_ref[x, f] * (moved + flow)
            carry[x] = carry[x] + cosine * flux
            carry[SUB + x] = carry[SUB + x] + sine * flux
            carry[2 * SUB + x] = carry[2 * SUB + x] + cosine * drift
            carry[3 * SUB + x] = carry[3 * SUB + x] + sine * drift
        return tuple(carry)

    for x in range(SUB):
        for f in range(groups):
            drift_ref[x, f] = freq[3, f] * r_ref[x, f]
    carry = lax.fori_loop(0, dirs, gather, (zero,) * (4 * SUB), unroll=2)

    total = []
    for j, value in enumerate(carry):
        if j < 2 * SUB:
            value = value * mask_b[j % SUB]
        total.append(jnp.sum(value, axis=0, keepdims=True))
    total.append(jnp.zeros((128 - 4 * SUB, 128), jnp.float32))
    stacked = jnp.concatenate(total, axis=0)
    lat = lax.broadcasted_iota(jnp.int32, (128, 128), 0)
    pick = (lat == bands[...]).astype(jnp.float32)
    picked = jnp.dot(stacked, pick, precision=lax.Precision.HIGHEST,
                     preferred_element_type=jnp.float32)
    rows[...] = picked.T
    band = 128 // n
    for k in range(n):
        sends[k] = rows[pl.ds(k * band, band), :]

    def exchange(i):
        target = lax.rem(me + i, n)
        return pltpu.make_async_remote_copy(
            src_ref=sends.at[target], dst_ref=recv.at[me], send_sem=a_ssem.at[i],
            recv_sem=a_rsem.at[i], device_id={"gx": target},
            device_id_type=pl.DeviceIdType.MESH)

    def begin(i, _):
        exchange(i).start()
        return 0

    def finish(i, _):
        exchange(i).wait()
        return 0

    lax.fori_loop(1, n, begin, 0)
    recv[pl.ds(me, 1)] = sends[pl.ds(me, 1)]

    def write(d, _):
        for f in range(groups):
            for x in range(SUB):
                at = (d * groups + f) * SUB + x
                moved = w_ref[at]
                out[pl.ds((d * groups + f) * SUB * SUB + x, SUB, stride=SUB), :] = (
                    moved * (1.0 + g_ref[at]) * r_ref[x, f])
        return 0

    lax.fori_loop(0, dirs, write, 0, unroll=2)
    lax.fori_loop(1, n, finish, 0)


def finish_kernel(n, parts, out, recv, after, ocean_out, ocean, sem):
    rows = out.shape[0] // parts
    copies = []
    for q in range(parts):
        part = pl.ds(q * rows, rows)
        copies.append(pltpu.make_async_copy(out.at[part], after.at[part], sem.at[q]))
        copies[-1].start()
    band = 128 // n
    per_tile = 128 // SUB
    block = lax.broadcasted_iota(jnp.int32, (band, 128), 1) // SUB
    for tile in range(max(1, n // per_tile)):
        for c in range(4):
            built = jnp.zeros((band, 128), jnp.float32)
            for k in range(min(n, per_tile)):
                moved = pltpu.roll(recv[tile * per_tile + k], (SUB * (k - c)) % 128, 1)
                built = jnp.where(block == k, moved, built)
            ocean[c, :, tile * 128:(tile + 1) * 128] = built
    copies.append(pltpu.make_async_copy(ocean, ocean_out, sem.at[parts]))
    copies[-1].start()
    for copy in copies:
        copy.wait()


def per_device(n, spectrum, wind, land_sea, band_rows):
    dirs, freqs, columns, lats = spectrum.shape
    groups = freqs // SUB
    half = dirs // 2 * groups * SUB
    band = lats // n
    f32 = jnp.float32
    anywhere = pl.BlockSpec(memory_space=pltpu.HBM)
    vmem = pl.BlockSpec(memory_space=pltpu.VMEM)
    cells = dirs * groups * SUB
    after, recv = pl.pallas_call(
        functools.partial(kernel, n, dirs, groups),
        out_shape=(pltpu.VMEM((cells * SUB, lats), f32), pltpu.VMEM((n, band, 128), f32)),
        in_specs=[anywhere] * 4,
        out_specs=(vmem, vmem),
        scratch_shapes=[
            pltpu.SMEM((2, dirs), f32),
            pltpu.VMEM((4, groups, SUB, lats), f32),
            pltpu.VMEM((2, SUB, lats), f32),
            pltpu.VMEM((SUB, lats), jnp.int32),
            pltpu.VMEM((1, lats), jnp.int32),
            pltpu.VMEM((cells, SUB, lats), f32),
            pltpu.VMEM((cells, SUB, lats), f32),
            pltpu.VMEM((cells, SUB, lats), f32),
            pltpu.VMEM((3, half, lats), f32),
            pltpu.VMEM((3, half, lats), f32),
            pltpu.VMEM((3, half, lats), f32),
            pltpu.VMEM((3, half, lats), f32),
            pltpu.VMEM((2, 2, SUB, lats), f32),
            pltpu.VMEM((2, SUB, lats), jnp.int32),
            pltpu.VMEM((2, 12, SUB, lats), f32),
            pltpu.VMEM((12, SUB, lats), f32),
            pltpu.VMEM((16, groups, SUB, lats), f32),
            pltpu.VMEM((SUB, groups, SUB, lats), f32),
            pltpu.VMEM((2, SUB, lats), f32),
            pltpu.VMEM((2, 2, SUB, lats), f32),
            pltpu.VMEM((128, 128), f32),
            pltpu.VMEM((n, band, 128), f32),
            pltpu.SemaphoreType.DMA((4,)),
            pltpu.SemaphoreType.DMA((3,)),
            pltpu.SemaphoreType.DMA((3, 3)),
            pltpu.SemaphoreType.DMA((14,)),
            pltpu.SemaphoreType.DMA((14,)),
            pltpu.SemaphoreType.DMA((n,)),
            pltpu.SemaphoreType.DMA((n,)),
        ],
        compiler_params=pltpu.CompilerParams(
            collective_id=0, has_side_effects=True, vmem_limit_bytes=48 * 2**20),
        name="wave_window",
    )(*[pltpu.with_memory_space_constraint(a, pltpu.HBM) for a in (
        spectrum.reshape(cells, SUB, lats), wind, land_sea, band_rows.reshape(1, lats))])
    parts = 4
    after, ocean = pl.pallas_call(
        functools.partial(finish_kernel, n, parts),
        out_shape=(jax.ShapeDtypeStruct((cells * SUB, lats), f32),
                   jax.ShapeDtypeStruct((4, band, columns * n), f32)),
        in_specs=[vmem, vmem],
        out_specs=(anywhere, anywhere),
        scratch_shapes=[pltpu.VMEM((4, band, columns * n), f32), pltpu.SemaphoreType.DMA((parts + 1,))],
        compiler_params=pltpu.CompilerParams(vmem_limit_bytes=2**20),
        name="hand_over",
    )(after, recv)
    return after.reshape(spectrum.shape), ocean


def solution(mesh):
    placed = (
        P(None, None, ("member", "gx"), None),
        P(None, ("member", "gx"), None),
        P("gx", None),
        P(),
    )
    return jax.shard_map(
        functools.partial(per_device, mesh.shape["gx"]),
        mesh=mesh,
        in_specs=placed,
        out_specs=(P(None, None, ("member", "gx"), None), P(None, "gx", "member")),
        check_vma=False,
    )
```

```python
import functools
import math

import jax
import jax.numpy as jnp
from jax import lax
from jax.experimental import pallas as pl
from jax.experimental.pallas import tpu as pltpu
from jax.sharding import PartitionSpec as P

STEPS = 3
SUB = 8
LEFT, RIGHT = 8, 10


def kernel(n, dirs, groups, spec, wind_in, land_in, bands_in, out, recv,
           trig, freq, wind, land, bands, x_ref, w_ref, g_ref, send, halo, wind_h, land_h,
           wind_b, mask_b, r_ref, drift_ref, e_send, e_halo, rows, sends, coef,
           in_sem, small_sem, col_sem, meet, bulk_s, bulk_r, small_s, small_r, e_s, e_r, a_s, a_r):
    me = lax.axis_index("gx")
    right, left = lax.rem(me + 1, n), lax.rem(me + n - 1, n)
    late = lax.rem((me + 1) // 2, 2) == 0

    def greet(semaphore, reach):
        for peer in (lax.rem(me + reach, n), lax.rem(me + n - reach, n)):
            pl.semaphore_signal(semaphore, inc=1, device_id={"gx": peer},
                                device_id_type=pl.DeviceIdType.MESH)

    barrier = pltpu.get_barrier_semaphore()
    greet(barrier, 1)
    reaches = [2 ** i for i in range((n // 2 - 1).bit_length())]
    quarter = dirs // 4
    qbins = quarter * groups * SUB
    cells = dirs * groups * SUB
    lane = lax.broadcasted_iota(jnp.int32, (SUB, 128), 1)
    x_rows = x_ref.reshape(cells * SUB, 128)

    in_copy = pltpu.make_async_copy(spec, x_ref, in_sem.at[0])

    def column_copies(k):
        return [pltpu.make_async_copy(
            spec.at[pl.ds(first, bins), column], send.at[k, side, pl.ds(to, bins)], col_sem.at[k])
            for first, bins, side, to, column in [
                (0, qbins, 0, 0, SUB - 1 - k), (3 * qbins, qbins, 0, qbins, SUB - 1 - k),
                (qbins, 2 * qbins, 1, 0, k)]]

    def columns_here(k):
        pltpu.make_async_copy(send.at[k], halo.at[k], col_sem.at[k]).wait()

    tables_in = [pltpu.make_async_copy(src, dst, small_sem.at[i]) for i, (src, dst) in enumerate(
        [(wind_in, wind), (land_in, land), (bands_in, bands)])]
    columns_in = [column_copies(k) for k in range(3)]
    for copy in columns_in[0] + tables_in:
        copy.start()
    in_copy.start()
    for copy in columns_in[1] + columns_in[2]:
        copy.start()

    for d in range(dirs):
        angle = (d + 0.5) * (2.0 * math.pi / dirs)
        trig[0, d] = jnp.float32(math.cos(angle))
        trig[1, d] = jnp.float32(math.sin(angle))
    freqs = groups * SUB
    for f in range(groups):
        level = (lax.broadcasted_iota(jnp.int32, (SUB, 128), 0) + f * SUB).astype(jnp.float32)
        weight = (level + 1.0) * (1.0 / freqs)
        grown = jnp.exp(level * math.log(1.1))
        freq[0, f] = 0.45 / grown
        freq[1, f] = grown * (2.0 * math.pi * 0.0418 / 9.81)
        freq[2, f] = 0.3 * weight * weight
        freq[3, f] = weight * (3.0 / math.sqrt(dirs * freqs))

    def remote(src, dst, send_sem, recv_sem, target):
        return pltpu.make_async_remote_copy(
            src_ref=src, dst_ref=dst, send_sem=send_sem, recv_sem=recv_sem,
            device_id={"gx": target}, device_id_type=pl.DeviceIdType.MESH)

    def arrived(ref, sem):
        pltpu.make_async_copy(ref, ref, sem).wait()

    bulk = [[remote(send.at[k, side], halo.at[k, side], bulk_s.at[0], bulk_r.at[k],
                    (right, left)[side]) for side in range(2)] for k in range(3)]
    small = [remote(src, dst.at[side], small_s.at[j], small_r.at[j], (right, left)[side])
             for j, (src, dst) in enumerate([(wind, wind_h), (land, land_h)]) for side in range(2)]
    energy_msg = [[remote(e_send.at[s], e_halo.at[s, side], e_s.at[s], e_r.at[s],
                          (right, left)[side]) for side in range(2)] for s in range(2)]

    columns_here(0)
    pl.semaphore_wait(barrier, 2)
    for copy in bulk[0]:
        copy.start()
    if reaches:
        greet(meet.at[0], reaches[0])
    for copy in tables_in:
        copy.wait()

    def spread(slot, wind_tile, land_tile, column):
        for c in range(2):
            wind_b[c, slot] = jnp.broadcast_to(wind_tile[c][column:column + 1], (SUB, 128))
        mask_b[slot] = jnp.broadcast_to(
            land_tile[column:column + 1].astype(jnp.float32), (SUB, 128))

    own_wind = [wind[0], wind[1]]
    own_land = land[...]
    for x in range(SUB):
        spread(x, own_wind, own_land, x)

    for copy in small:
        copy.start()
    columns_here(1)
    columns_here(2)

    def launch(k, when):
        @pl.when(when)
        def _():
            for copy in bulk[k]:
                copy.start()

    def spread_word(rounds):
        for i in rounds:
            pl.semaphore_wait(meet.at[i], 2)
            if i + 1 < len(reaches):
                greet(meet.at[i + 1], reaches[i + 1])

    for copy in bulk[1]:
        copy.start()
    in_copy.wait()

    def scalars(d):
        return trig[0, d], trig[1, d]

    halves = [(0, 2 * quarter, True), (quarter, 0, False)]

    def coefficients(cosine, sine, f, east, turn):
        k = freq[0, f]
        along_x = k * (cosine if east else -cosine)
        along_y = k * jnp.abs(sine)
        centre = 1.0 - along_x - along_y
        return centre, along_x, jnp.where(lane == 127 * turn, 0.0, along_y)

    def shifted(value, turn):
        return pltpu.roll(value, 1 + 126 * turn, 1)

    def growth_of(cosine, sine, f, slot):
        ratio = (wind_b[0, slot] * cosine + wind_b[1, slot] * sine) * freq[1, f]
        return 0.05 * jnp.minimum(jnp.maximum(ratio - 1.0, 0.0), 4.0)

    zero = jnp.zeros((SUB, 128), jnp.float32)

    def main(step, sums):
        for d0, skip, east in halves:
            def body(i, sums, d0=d0, skip=skip, east=east):
                turn = i // quarter
                d = d0 + i + skip * turn
                cosine, sine = scalars(d)
                sums = list(sums)
                if step == 0:
                    speed = [wind_b[0, x] * cosine + wind_b[1, x] * sine for x in range(SUB)]
                for f in range(groups):
                    centre, along_x, along_y = coefficients(cosine, sine, f, east, turn)
                    before = None
                    for x in (range(SUB) if east else range(SUB - 1, -1, -1)):
                        at = (d * groups + f) * SUB + x
                        if step == 0:
                            value = x_rows[pl.ds((d * groups + f) * SUB * SUB + x, SUB, stride=SUB), :]
                            g_ref[at] = 0.05 * jnp.minimum(
                                jnp.maximum(speed[x] * freq[1, f] - 1.0, 0.0), 4.0)
                        else:
                            value = w_ref[at] * (1.0 + g_ref[at]) * r_ref[x, f]
                        new = centre * value + along_y * shifted(value, turn)
                        if before is not None:
                            new = new + along_x * before
                        before = value
                        w_ref[at] = new
                        sums[x] = sums[x] + new
                return tuple(sums)

            sums = lax.fori_loop(0, 2 * quarter, body, tuple(sums), unroll=2)
        return sums

    def edges():
        for side, (d0, skip, east) in enumerate(halves):
            yield side, d0, skip, east, (LEFT if east else RIGHT), (0 if east else SUB - 1)

    def over_tiles(body, carry, unroll=3):
        return lax.fori_loop(0, 2 * quarter, body, carry, unroll=unroll)

    def prepare(step):
        for side, d0, skip, east, slot, edge in edges():
            def body(i, carry, d0=d0, skip=skip, east=east, side=side, slot=slot):
                turn = i // quarter
                d = d0 + i + skip * turn
                cosine, sine = scalars(d)
                for f in range(groups):
                    centre, along_x, along_y = coefficients(cosine, sine, f, east, turn)
                    at = pl.ds((i * groups + f) * SUB, SUB)

                    def local(k, depth):
                        value = halo[k, side, at, :]
                        grown = 1.0 + growth_of(cosine, sine, f, slot + depth)
                        return (centre * value + along_y * shifted(value, turn)), grown

                    near, grown = local(0, 0)
                    if step == 1:
                        halo[0, side, at, :] = near * grown
                        coef[side, at, :] = along_x * grown
                    else:
                        far, grown_far = local(1, 1)
                        grown = along_x * grown
                        reach = along_x * grown_far * r_ref[slot + 1, f]
                        halo[0, side, at, :] = grown * (near + reach * far)
                        coef[side, at, :] = grown * reach * along_x
                return carry

            over_tiles(body, 0)

    def fix(step, sums):
        totals = {}
        for side, d0, skip, east, slot, edge in edges():
            def body(i, total, d0=d0, skip=skip, east=east, side=side, slot=slot, edge=edge):
                turn = i // quarter
                d = d0 + i + skip * turn
                cosine, _ = scalars(d)
                for f in range(groups):
                    at = pl.ds((i * groups + f) * SUB, SUB)
                    along_x = freq[0, f] * (cosine if east else -cosine)
                    if step == 0:
                        extra = along_x * halo[0, side, at, :]
                    else:
                        flow = r_ref[slot + 4 * (step - 1), f] * (
                            halo[0, side, at, :] + coef[side, at, :] * halo[step, side, at, :])
                        if step == 1:
                            halo[0, side, at, :] = flow
                            extra = along_x * flow
                        else:
                            extra = flow
                    cell = (d * groups + f) * SUB + edge
                    w_ref[cell] = w_ref[cell] + extra
                    total = total + extra
                return total

            totals[edge] = over_tiles(body, sums[edge])
        return tuple(totals.get(x, sums[x]) for x in range(SUB))

    def energy_rows(sums, which):
        return [jnp.sum(sums[x] * mask_b[x], axis=0, keepdims=True) for x in which]

    def energy_tile(sums):
        return jnp.concatenate(energy_rows(sums, range(SUB)), axis=0) * (1.0 / cells)

    def factor(tile, column, mask_slot, slot):
        ratio = jnp.broadcast_to(tile[column:column + 1], (SUB, 128))
        for f in range(groups):
            r_ref[slot, f] = mask_b[mask_slot] / (1.0 + freq[2, f] * ratio)

    def own_factors(tile):
        ratio = tile / (0.5 + tile)
        for x in range(SUB):
            factor(ratio, x, x, x)

    inner, outer = list(range(1, SUB - 1)), [0, SUB - 1]

    def gathered(which, sums):
        for x, row in zip(which, energy_rows(sums, which)):
            tile = row * (1.0 / cells)
            ratio = jnp.broadcast_to(tile / (0.5 + tile), (SUB, 128))
            for f in range(groups):
                value = mask_b[x] / (1.0 + freq[2, f] * ratio)
                r_ref[x, f] = value
                drift_ref[x, f] = freq[3, f] * value

        def gather(d, carry):
            cosine, sine = scalars(d)
            carry = list(carry)
            m = len(which)
            for j, x in enumerate(which):
                flux, drift = zero, zero
                for f in range(groups):
                    at = (d * groups + f) * SUB + x
                    moved = w_ref[at]
                    flow = g_ref[at] * moved
                    flux = flux + freq[3, f] * flow
                    drift = drift + drift_ref[x, f] * (moved + flow)
                carry[j] = carry[j] + cosine * flux
                carry[m + j] = carry[m + j] + sine * flux
                carry[2 * m + j] = carry[2 * m + j] + cosine * drift
                carry[3 * m + j] = carry[3 * m + j] + sine * drift
            return tuple(carry)

        return lax.fori_loop(0, dirs, gather, (zero,) * (4 * len(which)), unroll=2)

    sums = main(0, (zero,) * SUB)
    spread_word(range(0, 1) if reaches else [])
    arrived(halo.at[0], bulk_r.at[0])
    sums = fix(0, sums)
    for step in (1, 2):
        tile = energy_tile(sums)
        e_send[step - 1] = tile
        own_factors(tile)
        for copy in energy_msg[step - 1]:
            copy.start()
        launch(2, late if step == 2 else jnp.logical_not(late))
        sums = main(step, (zero,) * SUB)
        if step == 1:
            spread_word(range(1, min(2, len(reaches))))
            arrived(wind_h, small_r.at[0])
            arrived(land_h, small_r.at[1])
            for side in range(2):
                tiles = [wind_h[side, 0], wind_h[side, 1]]
                land_tile = land_h[side]
                for depth in range(2):
                    spread((LEFT if side == 0 else RIGHT) + depth, tiles, land_tile,
                           SUB - 1 - depth if side == 0 else depth)
        else:
            spread_word(range(2, len(reaches)))
        prepare(step)
        if step == 2:
            inner_sums = gathered(inner, sums)
        arrived(halo.at[step], bulk_r.at[step])
        arrived(e_halo.at[step - 1], e_r.at[step - 1])
        for side in range(2):
            seen = e_halo[step - 1, side]
            ratio = seen / (0.5 + seen)
            base = LEFT if side == 0 else RIGHT
            for depth in range(3 - step):
                factor(ratio, SUB - 1 - depth if side == 0 else depth, base + depth,
                       base + depth + 4 * (step - 1))
        sums = fix(step, sums)

    outer_sums = gathered(outer, sums)
    both = {}
    for which, parts in ((inner, inner_sums), (outer, outer_sums)):
        for c in range(4):
            for j, x in enumerate(which):
                both[c * SUB + x] = parts[c * len(which) + j]
    carry = [both[j] for j in range(4 * SUB)]

    total = []
    for j, value in enumerate(carry):
        if j < 2 * SUB:
            value = value * mask_b[j % SUB]
        total.append(jnp.sum(value, axis=0, keepdims=True))
    total.append(jnp.zeros((128 - 4 * SUB, 128), jnp.float32))
    stacked = jnp.concatenate(total, axis=0)
    lat = lax.broadcasted_iota(jnp.int32, (128, 128), 0)
    pick = (lat == bands[...]).astype(jnp.float32)
    picked = jnp.dot(stacked, pick, precision=lax.Precision.HIGHEST,
                     preferred_element_type=jnp.float32)
    rows[...] = picked.T
    band = 128 // n
    for k in range(n):
        sends[k] = rows[pl.ds(k * band, band), :]

    def begin(i, _):
        target = lax.rem(me + i, n)
        remote(sends.at[target], recv.at[me], a_s.at[0], a_r.at[0], target).start()
        return 0

    lax.fori_loop(1, n, begin, 0)
    recv[pl.ds(me, 1)] = sends[pl.ds(me, 1)]

    def write(d, _):
        for f in range(groups):
            for x in range(SUB):
                at = (d * groups + f) * SUB + x
                moved = w_ref[at]
                out[pl.ds((d * groups + f) * SUB * SUB + x, SUB, stride=SUB), :] = (
                    moved * (1.0 + g_ref[at]) * r_ref[x, f])
        return 0

    lax.fori_loop(0, dirs, write, 0, unroll=2)
    arrived(send, bulk_s.at[0])
    arrived(wind_h, small_s.at[0])
    arrived(land_h, small_s.at[1])
    for s in range(2):
        arrived(e_halo.at[s], e_s.at[s])
    others = sends.at[pl.ds(0, n - 1)]
    arrived(others, a_s.at[0])
    arrived(others, a_r.at[0])


def finish_kernel(n, parts, out, recv, after, ocean_out, ocean, sem):
    rows = out.shape[0] // parts
    copies = []
    for q in range(parts):
        part = pl.ds(q * rows, rows)
        copies.append(pltpu.make_async_copy(out.at[part], after.at[part], sem.at[q]))
        copies[-1].start()
    band = 128 // n
    per_tile = 128 // SUB
    block = lax.broadcasted_iota(jnp.int32, (band, 128), 1) // SUB
    for tile in range(max(1, n // per_tile)):
        for c in range(4):
            built = jnp.zeros((band, 128), jnp.float32)
            for k in range(min(n, per_tile)):
                moved = pltpu.roll(recv[tile * per_tile + k], (SUB * (k - c)) % 128, 1)
                built = jnp.where(block == k, moved, built)
            ocean[c, :, tile * 128:(tile + 1) * 128] = built
    copies.append(pltpu.make_async_copy(ocean, ocean_out, sem.at[parts]))
    copies[-1].start()
    for copy in copies:
        copy.wait()


def per_device(n, spectrum, wind, land_sea, band_rows):
    dirs, freqs, columns, lats = spectrum.shape
    groups = freqs // SUB
    half = dirs // 2 * groups * SUB
    band = lats // n
    f32 = jnp.float32
    anywhere = pl.BlockSpec(memory_space=pltpu.HBM)
    vmem = pl.BlockSpec(memory_space=pltpu.VMEM)
    cells = dirs * groups * SUB
    after, recv = pl.pallas_call(
        functools.partial(kernel, n, dirs, groups),
        out_shape=(pltpu.VMEM((cells * SUB, lats), f32), pltpu.VMEM((n, band, 128), f32)),
        in_specs=[anywhere] * 4,
        out_specs=(vmem, vmem),
        scratch_shapes=[
            pltpu.SMEM((2, dirs), f32),
            pltpu.VMEM((4, groups, SUB, lats), f32),
            pltpu.VMEM((2, SUB, lats), f32),
            pltpu.VMEM((SUB, lats), jnp.int32),
            pltpu.VMEM((1, lats), jnp.int32),
            pltpu.VMEM((cells, SUB, lats), f32),
            pltpu.VMEM((cells, SUB, lats), f32),
            pltpu.VMEM((cells, SUB, lats), f32),
            pltpu.VMEM((3, 2, half, lats), f32),
            pltpu.VMEM((3, 2, half, lats), f32),
            pltpu.VMEM((2, 2, SUB, lats), f32),
            pltpu.VMEM((2, SUB, lats), jnp.int32),
            pltpu.VMEM((2, 12, SUB, lats), f32),
            pltpu.VMEM((12, SUB, lats), f32),
            pltpu.VMEM((16, groups, SUB, lats), f32),
            pltpu.VMEM((SUB, groups, SUB, lats), f32),
            pltpu.VMEM((2, SUB, lats), f32),
            pltpu.VMEM((2, 2, SUB, lats), f32),
            pltpu.VMEM((128, 128), f32),
            pltpu.VMEM((n, band, 128), f32),
            pltpu.VMEM((2, half, lats), f32),
            pltpu.SemaphoreType.DMA((1,)),
            pltpu.SemaphoreType.DMA((3,)),
            pltpu.SemaphoreType.DMA((3,)),
            pltpu.SemaphoreType.REGULAR((max(1, (n // 2 - 1).bit_length()),)),
            pltpu.SemaphoreType.DMA((1,)),
            pltpu.SemaphoreType.DMA((3,)),
            pltpu.SemaphoreType.DMA((2,)),
            pltpu.SemaphoreType.DMA((2,)),
            pltpu.SemaphoreType.DMA((2,)),
            pltpu.SemaphoreType.DMA((2,)),
            pltpu.SemaphoreType.DMA((1,)),
            pltpu.SemaphoreType.DMA((1,)),
        ],
        compiler_params=pltpu.CompilerParams(
            collective_id=0, has_side_effects=True, vmem_limit_bytes=48 * 2**20),
        name="wave_window",
    )(*[pltpu.with_memory_space_constraint(a, pltpu.HBM) for a in (
        spectrum.reshape(cells, SUB, lats), wind, land_sea, band_rows.reshape(1, lats))])
    parts = 4
    after, ocean = pl.pallas_call(
        functools.partial(finish_kernel, n, parts),
        out_shape=(jax.ShapeDtypeStruct((cells * SUB, lats), f32),
                   jax.ShapeDtypeStruct((4, band, columns * n), f32)),
        in_specs=[vmem, vmem],
        out_specs=(anywhere, anywhere),
        scratch_shapes=[pltpu.VMEM((4, band, columns * n), f32), pltpu.SemaphoreType.DMA((parts + 1,))],
        compiler_params=pltpu.CompilerParams(vmem_limit_bytes=2**20),
        name="hand_over",
    )(after, recv)
    return after.reshape(spectrum.shape), ocean


def solution(mesh):
    placed = (
        P(None, None, ("member", "gx"), None),
        P(None, ("member", "gx"), None),
        P("gx", None),
        P(),
    )
    return jax.shard_map(
        functools.partial(per_device, mesh.shape["gx"]),
        mesh=mesh,
        in_specs=placed,
        out_specs=(P(None, None, ("member", "gx"), None), P(None, "gx", "member")),
        check_vma=False,
    )
```

```python
import functools
import math

import jax
import jax.numpy as jnp
from jax import lax
from jax.experimental import pallas as pl
from jax.experimental.pallas import tpu as pltpu
from jax.sharding import PartitionSpec as P

STEPS = 3
SUB = 8
LEFT, RIGHT = 8, 10


def kernel(n, dirs, groups, spec, wind_in, land_in, bands_in, out, recv,
           trig, freq, wind, land, bands, x_ref, w_ref, g_ref, send, halo, wind_h, land_h,
           wind_b, mask_b, r_ref, drift_ref, e_send, e_halo, rows, sends, coef, table, grow_h,
           in_sem, small_sem, col_sem, meet, bulk_s, bulk_r, small_s, small_r, e_s, e_r, a_s, a_r):
    me = lax.axis_index("gx")
    right, left = lax.rem(me + 1, n), lax.rem(me + n - 1, n)
    late = lax.rem((me + 1) // 2, 2) == 0

    def greet(semaphore, reach):
        for peer in (lax.rem(me + reach, n), lax.rem(me + n - reach, n)):
            pl.semaphore_signal(semaphore, inc=1, device_id={"gx": peer},
                                device_id_type=pl.DeviceIdType.MESH)

    barrier = pltpu.get_barrier_semaphore()
    greet(barrier, 1)
    reaches = [2 ** i for i in range((n // 2 - 1).bit_length())]
    quarter = dirs // 4
    qbins = quarter * groups * SUB
    cells = dirs * groups * SUB
    lane = lax.broadcasted_iota(jnp.int32, (SUB, 128), 1)
    x_rows = x_ref.reshape(cells * SUB, 128)

    in_copy = pltpu.make_async_copy(spec, x_ref, in_sem.at[0])

    def column_copies(k):
        return [pltpu.make_async_copy(
            spec.at[pl.ds(first, bins), column], send.at[k, side, pl.ds(to, bins)], col_sem.at[k])
            for first, bins, side, to, column in [
                (0, qbins, 0, 0, SUB - 1 - k), (3 * qbins, qbins, 0, qbins, SUB - 1 - k),
                (qbins, 2 * qbins, 1, 0, k)]]

    def columns_here(k):
        pltpu.make_async_copy(send.at[k], halo.at[k], col_sem.at[k]).wait()

    tables_in = [pltpu.make_async_copy(src, dst, small_sem.at[i]) for i, (src, dst) in enumerate(
        [(wind_in, wind), (land_in, land), (bands_in, bands)])]
    columns_in = [column_copies(k) for k in range(3)]
    for copy in columns_in[0] + tables_in:
        copy.start()
    in_copy.start()
    for copy in columns_in[1] + columns_in[2]:
        copy.start()

    for d in range(dirs):
        angle = (d + 0.5) * (2.0 * math.pi / dirs)
        trig[0, d] = jnp.float32(math.cos(angle))
        trig[1, d] = jnp.float32(math.sin(angle))
    freqs = groups * SUB
    for f in range(groups):
        level = (lax.broadcasted_iota(jnp.int32, (SUB, 128), 0) + f * SUB).astype(jnp.float32)
        weight = (level + 1.0) * (1.0 / freqs)
        grown = jnp.exp(level * math.log(1.1))
        freq[0, f] = 0.45 / grown
        freq[1, f] = grown * (2.0 * math.pi * 0.0418 / 9.81)
        freq[2, f] = 0.3 * weight * weight
        freq[3, f] = weight * (3.0 / math.sqrt(dirs * freqs))

    def remote(src, dst, send_sem, recv_sem, target):
        return pltpu.make_async_remote_copy(
            src_ref=src, dst_ref=dst, send_sem=send_sem, recv_sem=recv_sem,
            device_id={"gx": target}, device_id_type=pl.DeviceIdType.MESH)

    def arrived(ref, sem):
        pltpu.make_async_copy(ref, ref, sem).wait()

    bulk = [[remote(send.at[k, side], halo.at[k, side], bulk_s.at[0], bulk_r.at[k],
                    (right, left)[side]) for side in range(2)] for k in range(3)]
    small = [remote(src, dst.at[side], small_s.at[j], small_r.at[j], (right, left)[side])
             for j, (src, dst) in enumerate([(wind, wind_h), (land, land_h)]) for side in range(2)]
    energy_msg = [[remote(e_send.at[s], e_halo.at[s, side], e_s.at[s], e_r.at[s],
                          (right, left)[side]) for side in range(2)] for s in range(2)]

    columns_here(0)
    pl.semaphore_wait(barrier, 2)
    for copy in tables_in:
        copy.wait()
    for copy in small + bulk[0]:
        copy.start()
    if reaches:
        greet(meet.at[0], reaches[0])

    def spread(slot, wind_tile, land_tile, column):
        for c in range(2):
            wind_b[c, slot] = jnp.broadcast_to(wind_tile[c][column:column + 1], (SUB, 128))
        mask_b[slot] = jnp.broadcast_to(
            land_tile[column:column + 1].astype(jnp.float32), (SUB, 128))

    own_wind = [wind[0], wind[1]]
    own_land = land[...]
    for x in range(SUB):
        spread(x, own_wind, own_land, x)

    columns_here(1)
    columns_here(2)

    def launch(k, when):
        @pl.when(when)
        def _():
            for copy in bulk[k]:
                copy.start()

    def spread_word(rounds):
        for i in rounds:
            pl.semaphore_wait(meet.at[i], 2)
            if i + 1 < len(reaches):
                greet(meet.at[i + 1], reaches[i + 1])

    for copy in bulk[1]:
        copy.start()
    in_copy.wait()

    def scalars(d):
        return trig[0, d], trig[1, d]

    halves = [(0, 2 * quarter, True), (quarter, 0, False)]

    def coefficients(cosine, sine, f, east, turn):
        k = freq[0, f]
        along_x = k * (cosine if east else -cosine)
        along_y = k * jnp.abs(sine)
        centre = 1.0 - along_x - along_y
        return centre, along_x, jnp.where(lane == 127 * turn, 0.0, along_y)

    def stencil(bin_tile):
        return table[0, bin_tile], table[1, bin_tile], table[2, bin_tile]

    def shifted(value, turn):
        return pltpu.roll(value, 1 + 126 * turn, 1)

    def growth_of(cosine, sine, f, slot):
        ratio = (wind_b[0, slot] * cosine + wind_b[1, slot] * sine) * freq[1, f]
        return 0.05 * jnp.minimum(jnp.maximum(ratio - 1.0, 0.0), 4.0)

    zero = jnp.zeros((SUB, 128), jnp.float32)

    def main(step, sums):
        for d0, skip, east in halves:
            def body(i, sums, d0=d0, skip=skip, east=east):
                turn = i // quarter
                d = d0 + i + skip * turn
                sums = list(sums)
                if step == 0:
                    cosine, sine = scalars(d)
                    speed = [wind_b[0, x] * cosine + wind_b[1, x] * sine for x in range(SUB)]
                for f in range(groups):
                    if step == 0:
                        centre, along_x, along_y = coefficients(cosine, sine, f, east, turn)
                        for c, value in enumerate((centre, along_x, along_y)):
                            table[c, d * groups + f] = value
                    else:
                        centre, along_x, along_y = stencil(d * groups + f)
                    before = None
                    for x in (range(SUB) if east else range(SUB - 1, -1, -1)):
                        at = (d * groups + f) * SUB + x
                        if step == 0:
                            value = x_rows[pl.ds((d * groups + f) * SUB * SUB + x, SUB, stride=SUB), :]
                            g_ref[at] = 1.0 + 0.05 * jnp.minimum(
                                jnp.maximum(speed[x] * freq[1, f] - 1.0, 0.0), 4.0)
                        else:
                            value = w_ref[at] * g_ref[at] * r_ref[x, f]
                        new = centre * value + along_y * shifted(value, turn)
                        if before is not None:
                            new = new + along_x * before
                        before = value
                        w_ref[at] = new
                        sums[x] = sums[x] + new
                return tuple(sums)

            sums = lax.fori_loop(0, 2 * quarter, body, tuple(sums), unroll=9)
        return sums

    def edges():
        for side, (d0, skip, east) in enumerate(halves):
            yield side, d0, skip, east, (LEFT if east else RIGHT), (0 if east else SUB - 1)

    def over_tiles(body, carry, unroll=3):
        return lax.fori_loop(0, 2 * quarter, body, carry, unroll=unroll)

    def grow_halo():
        for side, d0, skip, east, slot, edge in edges():
            def body(i, carry, d0=d0, skip=skip, side=side, slot=slot):
                d = d0 + i + skip * (i // quarter)
                cosine, sine = scalars(d)
                for f in range(groups):
                    for depth in range(2):
                        grow_h[side, depth, pl.ds((i * groups + f) * SUB, SUB), :] = (
                            1.0 + growth_of(cosine, sine, f, slot + depth))
                return carry

            over_tiles(body, 0)

    def prepare(step):
        for side, d0, skip, east, slot, edge in edges():
            def body(i, carry, d0=d0, skip=skip, east=east, side=side, slot=slot):
                turn = i // quarter
                d = d0 + i + skip * turn
                for f in range(groups):
                    centre, along_x, along_y = stencil(d * groups + f)
                    at = pl.ds((i * groups + f) * SUB, SUB)

                    def local(k, depth):
                        value = halo[k, side, at, :]
                        grown = grow_h[side, depth, at, :]
                        return (centre * value + along_y * shifted(value, turn)), grown

                    near, grown = local(0, 0)
                    if step == 1:
                        halo[0, side, at, :] = near * grown
                        coef[side, at, :] = along_x * grown
                    else:
                        far, grown_far = local(1, 1)
                        grown = along_x * grown
                        reach = along_x * grown_far * r_ref[slot + 1, f]
                        halo[0, side, at, :] = grown * (near + reach * far)
                        coef[side, at, :] = grown * reach * along_x
                return carry

            over_tiles(body, 0, 6)

    def fix(step, sums):
        totals = {}
        for side, d0, skip, east, slot, edge in edges():
            def body(i, total, d0=d0, skip=skip, east=east, side=side, slot=slot, edge=edge):
                d = d0 + i + skip * (i // quarter)
                for f in range(groups):
                    at = pl.ds((i * groups + f) * SUB, SUB)
                    along_x = table[1, d * groups + f]
                    if step == 0:
                        extra = along_x * halo[0, side, at, :]
                    else:
                        flow = r_ref[slot + 4 * (step - 1), f] * (
                            halo[0, side, at, :] + coef[side, at, :] * halo[step, side, at, :])
                        if step == 1:
                            halo[0, side, at, :] = flow
                            extra = along_x * flow
                        else:
                            extra = flow
                    cell = (d * groups + f) * SUB + edge
                    w_ref[cell] = w_ref[cell] + extra
                    total = total + extra
                return total

            totals[edge] = over_tiles(body, sums[edge], 6)
        return tuple(totals.get(x, sums[x]) for x in range(SUB))

    def energy_rows(sums, which):
        return [jnp.sum(sums[x] * mask_b[x], axis=0, keepdims=True) for x in which]

    def energy_tile(sums):
        return jnp.concatenate(energy_rows(sums, range(SUB)), axis=0) * (1.0 / cells)

    def factor(tile, column, mask_slot, slot):
        ratio = jnp.broadcast_to(tile[column:column + 1], (SUB, 128))
        for f in range(groups):
            r_ref[slot, f] = mask_b[mask_slot] / (1.0 + freq[2, f] * ratio)

    def own_factors(tile):
        ratio = tile / (0.5 + tile)
        for x in range(SUB):
            factor(ratio, x, x, x)

    inner, outer = list(range(1, SUB - 1)), [0, SUB - 1]

    def gathered(which, sums):
        for x, row in zip(which, energy_rows(sums, which)):
            tile = row * (1.0 / cells)
            ratio = jnp.broadcast_to(tile / (0.5 + tile), (SUB, 128))
            for f in range(groups):
                value = mask_b[x] / (1.0 + freq[2, f] * ratio)
                r_ref[x, f] = value
                drift_ref[x, f] = freq[3, f] * value

        def gather(d, carry):
            cosine, sine = scalars(d)
            carry = list(carry)
            m = len(which)
            for j, x in enumerate(which):
                flux, drift = zero, zero
                for f in range(groups):
                    at = (d * groups + f) * SUB + x
                    moved = w_ref[at]
                    grown = g_ref[at] * moved
                    flux = flux + freq[3, f] * (grown - moved)
                    drift = drift + drift_ref[x, f] * grown
                carry[j] = carry[j] + cosine * flux
                carry[m + j] = carry[m + j] + sine * flux
                carry[2 * m + j] = carry[2 * m + j] + cosine * drift
                carry[3 * m + j] = carry[3 * m + j] + sine * drift
            return tuple(carry)

        return lax.fori_loop(0, dirs, gather, (zero,) * (4 * len(which)), unroll=2)

    sums = main(0, (zero,) * SUB)
    spread_word(range(0, 1) if reaches else [])
    arrived(wind_h, small_r.at[0])
    arrived(land_h, small_r.at[1])
    for side in range(2):
        tiles = [wind_h[side, 0], wind_h[side, 1]]
        land_tile = land_h[side]
        for depth in range(2):
            spread((LEFT if side == 0 else RIGHT) + depth, tiles, land_tile,
                   SUB - 1 - depth if side == 0 else depth)
    grow_halo()
    arrived(halo.at[0], bulk_r.at[0])
    sums = fix(0, sums)
    for step in (1, 2):
        tile = energy_tile(sums)
        e_send[step - 1] = tile
        own_factors(tile)
        for copy in energy_msg[step - 1]:
            copy.start()
        launch(2, late if step == 2 else jnp.logical_not(late))
        sums = main(step, (zero,) * SUB)
        if step == 1:
            spread_word(range(1, min(2, len(reaches))))
        else:
            spread_word(range(2, len(reaches)))
        prepare(step)
        if step == 2:
            inner_sums = gathered(inner, sums)
        arrived(halo.at[step], bulk_r.at[step])
        arrived(e_halo.at[step - 1], e_r.at[step - 1])
        for side in range(2):
            seen = e_halo[step - 1, side]
            ratio = seen / (0.5 + seen)
            base = LEFT if side == 0 else RIGHT
            for depth in range(3 - step):
                factor(ratio, SUB - 1 - depth if side == 0 else depth, base + depth,
                       base + depth + 4 * (step - 1))
        sums = fix(step, sums)

    outer_sums = gathered(outer, sums)
    both = {}
    for which, parts in ((inner, inner_sums), (outer, outer_sums)):
        for c in range(4):
            for j, x in enumerate(which):
                both[c * SUB + x] = parts[c * len(which) + j]
    carry = [both[j] for j in range(4 * SUB)]

    total = []
    for j, value in enumerate(carry):
        if j < 2 * SUB:
            value = value * mask_b[j % SUB]
        total.append(jnp.sum(value, axis=0, keepdims=True))
    total.append(jnp.zeros((128 - 4 * SUB, 128), jnp.float32))
    stacked = jnp.concatenate(total, axis=0)
    lat = lax.broadcasted_iota(jnp.int32, (128, 128), 0)
    pick = (lat == bands[...]).astype(jnp.float32)
    picked = jnp.dot(stacked, pick, precision=lax.Precision.HIGHEST,
                     preferred_element_type=jnp.float32)
    rows[...] = picked.T
    band = 128 // n
    for k in range(n):
        sends[k] = rows[pl.ds(k * band, band), :]

    def begin(i, _):
        target = lax.rem(me + i, n)
        remote(sends.at[target], recv.at[me], a_s.at[0], a_r.at[0], target).start()
        return 0

    lax.fori_loop(1, n, begin, 0)
    recv[pl.ds(me, 1)] = sends[pl.ds(me, 1)]

    def write(d, _):
        for f in range(groups):
            for x in range(SUB):
                at = (d * groups + f) * SUB + x
                moved = w_ref[at]
                out[pl.ds((d * groups + f) * SUB * SUB + x, SUB, stride=SUB), :] = (
                    moved * g_ref[at] * r_ref[x, f])
        return 0

    lax.fori_loop(0, dirs, write, 0, unroll=2)
    arrived(send, bulk_s.at[0])
    arrived(wind_h, small_s.at[0])
    arrived(land_h, small_s.at[1])
    for s in range(2):
        arrived(e_halo.at[s], e_s.at[s])
    others = sends.at[pl.ds(0, n - 1)]
    arrived(others, a_s.at[0])
    arrived(others, a_r.at[0])


def finish_kernel(n, parts, out, recv, after, ocean_out, ocean, sem):
    rows = out.shape[0] // parts
    copies = []
    for q in range(parts):
        part = pl.ds(q * rows, rows)
        copies.append(pltpu.make_async_copy(out.at[part], after.at[part], sem.at[q]))
        copies[-1].start()
    band = 128 // n
    per_tile = 128 // SUB
    block = lax.broadcasted_iota(jnp.int32, (band, 128), 1) // SUB
    for tile in range(max(1, n // per_tile)):
        for c in range(4):
            built = jnp.zeros((band, 128), jnp.float32)
            for k in range(min(n, per_tile)):
                moved = pltpu.roll(recv[tile * per_tile + k], (SUB * (k - c)) % 128, 1)
                built = jnp.where(block == k, moved, built)
            ocean[c, :, tile * 128:(tile + 1) * 128] = built
    copies.append(pltpu.make_async_copy(ocean, ocean_out, sem.at[parts]))
    copies[-1].start()
    for copy in copies:
        copy.wait()


def per_device(n, spectrum, wind, land_sea, band_rows):
    dirs, freqs, columns, lats = spectrum.shape
    groups = freqs // SUB
    half = dirs // 2 * groups * SUB
    band = lats // n
    f32 = jnp.float32
    anywhere = pl.BlockSpec(memory_space=pltpu.HBM)
    vmem = pl.BlockSpec(memory_space=pltpu.VMEM)
    cells = dirs * groups * SUB
    after, recv = pl.pallas_call(
        functools.partial(kernel, n, dirs, groups),
        out_shape=(pltpu.VMEM((cells * SUB, lats), f32), pltpu.VMEM((n, band, 128), f32)),
        in_specs=[anywhere] * 4,
        out_specs=(vmem, vmem),
        scratch_shapes=[
            pltpu.SMEM((2, dirs), f32),
            pltpu.VMEM((4, groups, SUB, lats), f32),
            pltpu.VMEM((2, SUB, lats), f32),
            pltpu.VMEM((SUB, lats), jnp.int32),
            pltpu.VMEM((1, lats), jnp.int32),
            pltpu.VMEM((cells, SUB, lats), f32),
            pltpu.VMEM((cells, SUB, lats), f32),
            pltpu.VMEM((cells, SUB, lats), f32),
            pltpu.VMEM((3, 2, half, lats), f32),
            pltpu.VMEM((3, 2, half, lats), f32),
            pltpu.VMEM((2, 2, SUB, lats), f32),
            pltpu.VMEM((2, SUB, lats), jnp.int32),
            pltpu.VMEM((2, 12, SUB, lats), f32),
            pltpu.VMEM((12, SUB, lats), f32),
            pltpu.VMEM((16, groups, SUB, lats), f32),
            pltpu.VMEM((SUB, groups, SUB, lats), f32),
            pltpu.VMEM((2, SUB, lats), f32),
            pltpu.VMEM((2, 2, SUB, lats), f32),
            pltpu.VMEM((128, 128), f32),
            pltpu.VMEM((n, band, 128), f32),
            pltpu.VMEM((2, half, lats), f32),
            pltpu.VMEM((3, dirs * groups, SUB, lats), f32),
            pltpu.VMEM((2, 2, half, lats), f32),
            pltpu.SemaphoreType.DMA((1,)),
            pltpu.SemaphoreType.DMA((3,)),
            pltpu.SemaphoreType.DMA((3,)),
            pltpu.SemaphoreType.REGULAR((max(1, (n // 2 - 1).bit_length()),)),
            pltpu.SemaphoreType.DMA((1,)),
            pltpu.SemaphoreType.DMA((3,)),
            pltpu.SemaphoreType.DMA((2,)),
            pltpu.SemaphoreType.DMA((2,)),
            pltpu.SemaphoreType.DMA((2,)),
            pltpu.SemaphoreType.DMA((2,)),
            pltpu.SemaphoreType.DMA((1,)),
            pltpu.SemaphoreType.DMA((1,)),
        ],
        compiler_params=pltpu.CompilerParams(
            collective_id=0, has_side_effects=True, vmem_limit_bytes=48 * 2**20),
        name="wave_window",
    )(*[pltpu.with_memory_space_constraint(a, pltpu.HBM) for a in (
        spectrum.reshape(cells, SUB, lats), wind, land_sea, band_rows.reshape(1, lats))])
    parts = 4
    after, ocean = pl.pallas_call(
        functools.partial(finish_kernel, n, parts),
        out_shape=(jax.ShapeDtypeStruct((cells * SUB, lats), f32),
                   jax.ShapeDtypeStruct((4, band, columns * n), f32)),
        in_specs=[vmem, vmem],
        out_specs=(anywhere, anywhere),
        scratch_shapes=[pltpu.VMEM((4, band, columns * n), f32), pltpu.SemaphoreType.DMA((parts + 1,))],
        compiler_params=pltpu.CompilerParams(vmem_limit_bytes=2**20),
        name="hand_over",
    )(after, recv)
    return after.reshape(spectrum.shape), ocean


def solution(mesh):
    placed = (
        P(None, None, ("member", "gx"), None),
        P(None, ("member", "gx"), None),
        P("gx", None),
        P(),
    )
    return jax.shard_map(
        functools.partial(per_device, mesh.shape["gx"]),
        mesh=mesh,
        in_specs=placed,
        out_specs=(P(None, None, ("member", "gx"), None), P(None, "gx", "member")),
        check_vma=False,
    )
```

```python
import functools
import math

import jax
import jax.numpy as jnp
from jax import lax
from jax.experimental import pallas as pl
from jax.experimental.pallas import tpu as pltpu
from jax.sharding import PartitionSpec as P

STEPS = 3
SUB = 8
LEFT, RIGHT = 8, 10


def kernel(n, dirs, groups, spec, wind_in, land_in, bands_in, out, recv,
           trig, freq, wind, land, bands, x_ref, w_ref, g_ref, send, halo, wind_h, land_h,
           wind_b, mask_b, r_ref, drift_ref, e_send, e_halo, rows, sends, coef, table, grow_h,
           in_sem, small_sem, col_sem, meet, bulk_s, bulk_r, small_s, small_r, e_s, e_r, a_s, a_r):
    me = lax.axis_index("gx")
    right, left = lax.rem(me + 1, n), lax.rem(me + n - 1, n)
    late = lax.rem((me + 1) // 2, 2) == 0

    def greet(semaphore, reach):
        for peer in (lax.rem(me + reach, n), lax.rem(me + n - reach, n)):
            pl.semaphore_signal(semaphore, inc=1, device_id={"gx": peer},
                                device_id_type=pl.DeviceIdType.MESH)

    barrier = pltpu.get_barrier_semaphore()
    greet(barrier, 1)
    reaches = [2 ** i for i in range((n // 2 - 1).bit_length())]
    quarter = dirs // 4
    qbins = quarter * groups * SUB
    cells = dirs * groups * SUB
    lane = lax.broadcasted_iota(jnp.int32, (SUB, 128), 1)
    x_rows = x_ref.reshape(cells * SUB, 128)

    in_copy = pltpu.make_async_copy(spec, x_ref, in_sem.at[0])

    def column_copies(k):
        return [pltpu.make_async_copy(
            spec.at[pl.ds(first, bins), column], send.at[k, side, pl.ds(to, bins)], col_sem.at[k])
            for first, bins, side, to, column in [
                (0, qbins, 0, 0, SUB - 1 - k), (3 * qbins, qbins, 0, qbins, SUB - 1 - k),
                (qbins, 2 * qbins, 1, 0, k)]]

    def columns_here(k):
        pltpu.make_async_copy(send.at[k], halo.at[k], col_sem.at[k]).wait()

    tables_in = [pltpu.make_async_copy(src, dst, small_sem.at[i]) for i, (src, dst) in enumerate(
        [(wind_in, wind), (land_in, land), (bands_in, bands)])]
    columns_in = [column_copies(k) for k in range(3)]
    for copy in columns_in[0] + tables_in:
        copy.start()
    in_copy.start()
    for copy in columns_in[1] + columns_in[2]:
        copy.start()

    for d in range(dirs):
        angle = (d + 0.5) * (2.0 * math.pi / dirs)
        trig[0, d] = jnp.float32(math.cos(angle))
        trig[1, d] = jnp.float32(math.sin(angle))
    freqs = groups * SUB
    for f in range(groups):
        level = (lax.broadcasted_iota(jnp.int32, (SUB, 128), 0) + f * SUB).astype(jnp.float32)
        weight = (level + 1.0) * (1.0 / freqs)
        grown = jnp.exp(level * math.log(1.1))
        freq[0, f] = 0.45 / grown
        freq[1, f] = grown * (2.0 * math.pi * 0.0418 / 9.81)
        freq[2, f] = 0.3 * weight * weight
        freq[3, f] = weight * (3.0 / math.sqrt(dirs * freqs))

    def remote(src, dst, send_sem, recv_sem, target):
        return pltpu.make_async_remote_copy(
            src_ref=src, dst_ref=dst, send_sem=send_sem, recv_sem=recv_sem,
            device_id={"gx": target}, device_id_type=pl.DeviceIdType.MESH)

    def arrived(ref, sem):
        pltpu.make_async_copy(ref, ref, sem).wait()

    bulk = [[remote(send.at[k, side], halo.at[k, side], bulk_s.at[0], bulk_r.at[k],
                    (right, left)[side]) for side in range(2)] for k in range(3)]
    ends = (pl.ds(SUB - 2, 2), pl.ds(0, 2))
    small = [remote(src, dst, small_s.at[j], small_r.at[j], (right, left)[side])
             for side in range(2) for j, (src, dst) in enumerate([
                 (wind.at[:, ends[side]], wind_h.at[side, :, ends[side]]),
                 (land.at[ends[side]], land_h.at[side, ends[side]])])]
    energy_msg = [[remote(e_send.at[s, ends[side]], e_halo.at[s, side, ends[side]], e_s.at[s],
                          e_r.at[s], (right, left)[side]) for side in range(2)] for s in range(2)]
    wind_rows, land_rows = wind_h.at[:, :, ends[1]], land_h.at[:, ends[1]]

    columns_here(0)
    pl.semaphore_wait(barrier, 2)
    for copy in tables_in:
        copy.wait()
    for copy in small + bulk[0]:
        copy.start()
    if reaches:
        greet(meet.at[0], reaches[0])

    def spread(slot, wind_tile, land_tile, column):
        for c in range(2):
            wind_b[c, slot] = jnp.broadcast_to(wind_tile[c][column:column + 1], (SUB, 128))
        mask_b[slot] = jnp.broadcast_to(
            land_tile[column:column + 1].astype(jnp.float32), (SUB, 128))

    own_wind = [wind[0], wind[1]]
    own_land = land[...]
    for x in range(SUB):
        spread(x, own_wind, own_land, x)

    columns_here(1)
    columns_here(2)

    def launch(k, when):
        @pl.when(when)
        def _():
            for copy in bulk[k]:
                copy.start()

    def spread_word(rounds):
        for i in rounds:
            pl.semaphore_wait(meet.at[i], 2)
            if i + 1 < len(reaches):
                greet(meet.at[i + 1], reaches[i + 1])

    for copy in bulk[1]:
        copy.start()
    in_copy.wait()

    def scalars(d):
        return trig[0, d], trig[1, d]

    halves = [(0, 2 * quarter, True), (quarter, 0, False)]

    def coefficients(cosine, sine, f, east, turn):
        k = freq[0, f]
        along_x = k * (cosine if east else -cosine)
        along_y = k * jnp.abs(sine)
        centre = 1.0 - along_x - along_y
        return centre, along_x, jnp.where(lane == 127 * turn, 0.0, along_y)

    def stencil(bin_tile):
        return table[0, bin_tile], table[1, bin_tile], table[2, bin_tile]

    def shifted(value, turn):
        return pltpu.roll(value, 1 + 126 * turn, 1)

    def growth_of(cosine, sine, f, slot):
        ratio = (wind_b[0, slot] * cosine + wind_b[1, slot] * sine) * freq[1, f]
        return 0.05 * jnp.minimum(jnp.maximum(ratio - 1.0, 0.0), 4.0)

    zero = jnp.zeros((SUB, 128), jnp.float32)

    def main(step, sums):
        for d0, skip, east in halves:
            def body(i, sums, d0=d0, skip=skip, east=east):
                turn = i // quarter
                d = d0 + i + skip * turn
                sums = list(sums)
                if step == 0:
                    cosine, sine = scalars(d)
                    speed = [wind_b[0, x] * cosine + wind_b[1, x] * sine for x in range(SUB)]
                for f in range(groups):
                    if step == 0:
                        centre, along_x, along_y = coefficients(cosine, sine, f, east, turn)
                        for c, value in enumerate((centre, along_x, along_y)):
                            table[c, d * groups + f] = value
                    else:
                        centre, along_x, along_y = stencil(d * groups + f)
                    before = None
                    for x in (range(SUB) if east else range(SUB - 1, -1, -1)):
                        at = (d * groups + f) * SUB + x
                        if step == 0:
                            value = x_rows[pl.ds((d * groups + f) * SUB * SUB + x, SUB, stride=SUB), :]
                            g_ref[at] = 1.0 + 0.05 * jnp.minimum(
                                jnp.maximum(speed[x] * freq[1, f] - 1.0, 0.0), 4.0)
                        else:
                            value = w_ref[at] * g_ref[at] * r_ref[x, f]
                        new = centre * value + along_y * shifted(value, turn)
                        if before is not None:
                            new = new + along_x * before
                        before = value
                        w_ref[at] = new
                        sums[x] = sums[x] + new
                return tuple(sums)

            sums = lax.fori_loop(0, 2 * quarter, body, tuple(sums), unroll=9)
        return sums

    def edges():
        for side, (d0, skip, east) in enumerate(halves):
            yield side, d0, skip, east, (LEFT if east else RIGHT), (0 if east else SUB - 1)

    def over_tiles(body, carry, unroll=3):
        return lax.fori_loop(0, 2 * quarter, body, carry, unroll=unroll)

    def grow_halo():
        for side, d0, skip, east, slot, edge in edges():
            def body(i, carry, d0=d0, skip=skip, side=side, slot=slot):
                d = d0 + i + skip * (i // quarter)
                cosine, sine = scalars(d)
                for f in range(groups):
                    for depth in range(2):
                        grow_h[side, depth, pl.ds((i * groups + f) * SUB, SUB), :] = (
                            1.0 + growth_of(cosine, sine, f, slot + depth))
                return carry

            over_tiles(body, 0)

    def prepare(step):
        for side, d0, skip, east, slot, edge in edges():
            def body(i, carry, d0=d0, skip=skip, east=east, side=side, slot=slot):
                turn = i // quarter
                d = d0 + i + skip * turn
                for f in range(groups):
                    centre, along_x, along_y = stencil(d * groups + f)
                    at = pl.ds((i * groups + f) * SUB, SUB)

                    def local(k, depth):
                        value = halo[k, side, at, :]
                        grown = grow_h[side, depth, at, :]
                        return (centre * value + along_y * shifted(value, turn)), grown

                    near, grown = local(0, 0)
                    if step == 1:
                        halo[0, side, at, :] = near * grown
                        coef[side, at, :] = along_x * grown
                    else:
                        far, grown_far = local(1, 1)
                        grown = along_x * grown
                        reach = along_x * grown_far * r_ref[slot + 1, f]
                        halo[0, side, at, :] = grown * (near + reach * far)
                        coef[side, at, :] = grown * reach * along_x
                return carry

            over_tiles(body, 0, 6)

    def contribute(acc, d, moved, grown):
        cosine, sine = scalars(d)
        acc = list(acc)
        flux = zero
        for f in range(groups):
            flux = flux + freq[3, f] * (grown[f] - moved[f])
            acc[2 + f] = acc[2 + f] + cosine * grown[f]
            acc[2 + groups + f] = acc[2 + groups + f] + sine * grown[f]
        acc[0] = acc[0] + cosine * flux
        acc[1] = acc[1] + sine * flux
        return acc

    def fix(step, sums, parts=None):
        totals = {}
        for side, d0, skip, east, slot, edge in edges():
            def body(i, carry, d0=d0, skip=skip, side=side, slot=slot, edge=edge):
                total, acc = carry[0], carry[1:]
                d = d0 + i + skip * (i // quarter)
                moved, grown = [], []
                for f in range(groups):
                    at = pl.ds((i * groups + f) * SUB, SUB)
                    cell = (d * groups + f) * SUB + edge
                    if step == 0:
                        extra = table[1, d * groups + f] * halo[0, side, at, :]
                    else:
                        extra = r_ref[slot + 4 * (step - 1), f] * (
                            halo[0, side, at, :] + coef[side, at, :] * halo[step, side, at, :])
                        if step == 1:
                            halo[0, side, at, :] = extra
                            extra = table[1, d * groups + f] * extra
                    w_ref[cell] = w_ref[cell] + extra
                    total = total + extra
                    moved.append(extra)
                    if acc:
                        grown.append(g_ref[cell] * extra)
                if acc:
                    acc = contribute(acc, d, moved, grown)
                return (total, *acc)

            start = (sums[edge],) + (tuple(parts[edge]) if parts else ())
            done = over_tiles(body, start, 6)
            totals[edge] = done[0]
            if parts:
                parts[edge] = done[1:]
        return tuple(totals.get(x, sums[x]) for x in range(SUB))

    def energy_rows(sums, which):
        return [jnp.sum(sums[x] * mask_b[x], axis=0, keepdims=True) for x in which]

    def energy_tile(sums):
        return jnp.concatenate(energy_rows(sums, range(SUB)), axis=0) * (1.0 / cells)

    def factor(tile, column, mask_slot, slot):
        ratio = jnp.broadcast_to(tile[column:column + 1], (SUB, 128))
        for f in range(groups):
            r_ref[slot, f] = mask_b[mask_slot] / (1.0 + freq[2, f] * ratio)

    def own_factors(tile):
        ratio = tile / (0.5 + tile)
        for x in range(SUB):
            factor(ratio, x, x, x)

    inner, outer = list(range(1, SUB - 1)), [0, SUB - 1]

    def last_factors(which, sums):
        for x, row in zip(which, energy_rows(sums, which)):
            tile = row * (1.0 / cells)
            ratio = jnp.broadcast_to(tile / (0.5 + tile), (SUB, 128))
            for f in range(groups):
                r_ref[x, f] = mask_b[x] / (1.0 + freq[2, f] * ratio)

    def row_sums(which, values):
        rows_of = {}
        for c in range(4):
            for j, x in enumerate(which):
                value = values[c * len(which) + j]
                if c < 2:
                    value = value * mask_b[x]
                rows_of[c * SUB + x] = jnp.sum(value, axis=0, keepdims=True)
        return rows_of

    def gathered_outer():
        size = 2 + 2 * groups

        def gather(d, carry):
            done = []
            for j, x in enumerate(outer):
                cells_of = [(d * groups + f) * SUB + x for f in range(groups)]
                moved = [w_ref[at] for at in cells_of]
                grown = [g_ref[at] * value for at, value in zip(cells_of, moved)]
                done += contribute(carry[j * size:(j + 1) * size], d, moved, grown)
            return tuple(done)

        total = lax.fori_loop(0, dirs, gather, (zero,) * (2 * size), unroll=2)
        return {x: total[j * size:(j + 1) * size] for j, x in enumerate(outer)}

    def gathered(which, sums):
        last_factors(which, sums)
        for x in which:
            for f in range(groups):
                drift_ref[x, f] = freq[3, f] * r_ref[x, f]

        def gather(d, carry):
            cosine, sine = scalars(d)
            carry = list(carry)
            m = len(which)
            for j, x in enumerate(which):
                flux, drift = zero, zero
                for f in range(groups):
                    at = (d * groups + f) * SUB + x
                    moved = w_ref[at]
                    grown = g_ref[at] * moved
                    flux = flux + freq[3, f] * (grown - moved)
                    drift = drift + drift_ref[x, f] * grown
                carry[j] = carry[j] + cosine * flux
                carry[m + j] = carry[m + j] + sine * flux
                carry[2 * m + j] = carry[2 * m + j] + cosine * drift
                carry[3 * m + j] = carry[3 * m + j] + sine * drift
            return tuple(carry)

        return row_sums(which, lax.fori_loop(
            0, dirs, gather, (zero,) * (4 * len(which)), unroll=2))

    sums = main(0, (zero,) * SUB)
    spread_word(range(0, 1) if reaches else [])
    arrived(wind_rows, small_r.at[0])
    arrived(land_rows, small_r.at[1])
    for side in range(2):
        tiles = [wind_h[side, 0], wind_h[side, 1]]
        land_tile = land_h[side]
        for depth in range(2):
            spread((LEFT if side == 0 else RIGHT) + depth, tiles, land_tile,
                   SUB - 1 - depth if side == 0 else depth)
    grow_halo()
    arrived(halo.at[0], bulk_r.at[0])
    sums = fix(0, sums)
    outer_parts = None
    for step in (1, 2):
        tile = energy_tile(sums)
        e_send[step - 1] = tile
        own_factors(tile)
        for copy in energy_msg[step - 1]:
            copy.start()
        launch(2, late if step == 2 else jnp.logical_not(late))
        sums = main(step, (zero,) * SUB)
        if step == 1:
            spread_word(range(1, min(2, len(reaches))))
        else:
            spread_word(range(2, len(reaches)))
        prepare(step)
        if step == 2:
            inner_rows = gathered(inner, sums)
            outer_parts = gathered_outer()
        arrived(halo.at[step], bulk_r.at[step])
        arrived(e_halo.at[step - 1, :, ends[1]], e_r.at[step - 1])
        for side in range(2):
            seen = e_halo[step - 1, side]
            ratio = seen / (0.5 + seen)
            base = LEFT if side == 0 else RIGHT
            for depth in range(3 - step):
                factor(ratio, SUB - 1 - depth if side == 0 else depth, base + depth,
                       base + depth + 4 * (step - 1))
        sums = fix(step, sums, outer_parts)

    last_factors(outer, sums)
    values = [None] * 8
    for j, x in enumerate(outer):
        part = outer_parts[x]
        values[j], values[2 + j] = part[0], part[1]
        for c in range(2):
            drift = zero
            for f in range(groups):
                drift = drift + (freq[3, f] * r_ref[x, f]) * part[2 + c * groups + f]
            values[4 + 2 * c + j] = drift
    all_rows = {**inner_rows, **row_sums(outer, values)}
    total = [all_rows[j] for j in range(4 * SUB)]
    total.append(jnp.zeros((128 - 4 * SUB, 128), jnp.float32))
    stacked = jnp.concatenate(total, axis=0)
    lat = lax.broadcasted_iota(jnp.int32, (128, 128), 0)
    pick = (lat == bands[...]).astype(jnp.float32)
    picked = jnp.dot(stacked, pick, precision=lax.Precision.HIGHEST,
                     preferred_element_type=jnp.float32)
    rows[...] = picked.T
    band = 128 // n
    for k in range(n):
        sends[k] = rows[pl.ds(k * band, band), :]

    def begin(i, _):
        target = lax.rem(me + i, n)
        remote(sends.at[target], recv.at[me], a_s.at[0], a_r.at[0], target).start()
        return 0

    lax.fori_loop(1, n, begin, 0)
    recv[pl.ds(me, 1)] = sends[pl.ds(me, 1)]

    def write(d, _):
        for f in range(groups):
            for x in range(SUB):
                at = (d * groups + f) * SUB + x
                moved = w_ref[at]
                out[pl.ds((d * groups + f) * SUB * SUB + x, SUB, stride=SUB), :] = (
                    moved * g_ref[at] * r_ref[x, f])
        return 0

    lax.fori_loop(0, dirs, write, 0, unroll=2)
    arrived(send, bulk_s.at[0])
    arrived(wind_rows, small_s.at[0])
    arrived(land_rows, small_s.at[1])
    for s in range(2):
        arrived(e_halo.at[s, :, ends[1]], e_s.at[s])
    others = sends.at[pl.ds(0, n - 1)]
    arrived(others, a_s.at[0])
    arrived(others, a_r.at[0])


def finish_kernel(n, parts, out, recv, after, ocean_out, ocean, sem):
    rows = out.shape[0] // parts
    copies = []
    for q in range(parts):
        part = pl.ds(q * rows, rows)
        copies.append(pltpu.make_async_copy(out.at[part], after.at[part], sem.at[q]))
        copies[-1].start()
    band = 128 // n
    per_tile = 128 // SUB
    block = lax.broadcasted_iota(jnp.int32, (band, 128), 1) // SUB
    for tile in range(max(1, n // per_tile)):
        for c in range(4):
            built = jnp.zeros((band, 128), jnp.float32)
            for k in range(min(n, per_tile)):
                moved = pltpu.roll(recv[tile * per_tile + k], (SUB * (k - c)) % 128, 1)
                built = jnp.where(block == k, moved, built)
            ocean[c, :, tile * 128:(tile + 1) * 128] = built
    copies.append(pltpu.make_async_copy(ocean, ocean_out, sem.at[parts]))
    copies[-1].start()
    for copy in copies:
        copy.wait()


def per_device(n, spectrum, wind, land_sea, band_rows):
    dirs, freqs, columns, lats = spectrum.shape
    groups = freqs // SUB
    half = dirs // 2 * groups * SUB
    band = lats // n
    f32 = jnp.float32
    anywhere = pl.BlockSpec(memory_space=pltpu.HBM)
    vmem = pl.BlockSpec(memory_space=pltpu.VMEM)
    cells = dirs * groups * SUB
    after, recv = pl.pallas_call(
        functools.partial(kernel, n, dirs, groups),
        out_shape=(pltpu.VMEM((cells * SUB, lats), f32), pltpu.VMEM((n, band, 128), f32)),
        in_specs=[anywhere] * 4,
        out_specs=(vmem, vmem),
        scratch_shapes=[
            pltpu.SMEM((2, dirs), f32),
            pltpu.VMEM((4, groups, SUB, lats), f32),
            pltpu.VMEM((2, SUB, lats), f32),
            pltpu.VMEM((SUB, lats), jnp.int32),
            pltpu.VMEM((1, lats), jnp.int32),
            pltpu.VMEM((cells, SUB, lats), f32),
            pltpu.VMEM((cells, SUB, lats), f32),
            pltpu.VMEM((cells, SUB, lats), f32),
            pltpu.VMEM((3, 2, half, lats), f32),
            pltpu.VMEM((3, 2, half, lats), f32),
            pltpu.VMEM((2, 2, SUB, lats), f32),
            pltpu.VMEM((2, SUB, lats), jnp.int32),
            pltpu.VMEM((2, 12, SUB, lats), f32),
            pltpu.VMEM((12, SUB, lats), f32),
            pltpu.VMEM((16, groups, SUB, lats), f32),
            pltpu.VMEM((SUB, groups, SUB, lats), f32),
            pltpu.VMEM((2, SUB, lats), f32),
            pltpu.VMEM((2, 2, SUB, lats), f32),
            pltpu.VMEM((128, 128), f32),
            pltpu.VMEM((n, band, 128), f32),
            pltpu.VMEM((2, half, lats), f32),
            pltpu.VMEM((3, dirs * groups, SUB, lats), f32),
            pltpu.VMEM((2, 2, half, lats), f32),
            pltpu.SemaphoreType.DMA((1,)),
            pltpu.SemaphoreType.DMA((3,)),
            pltpu.SemaphoreType.DMA((3,)),
            pltpu.SemaphoreType.REGULAR((max(1, (n // 2 - 1).bit_length()),)),
            pltpu.SemaphoreType.DMA((1,)),
            pltpu.SemaphoreType.DMA((3,)),
            pltpu.SemaphoreType.DMA((2,)),
            pltpu.SemaphoreType.DMA((2,)),
            pltpu.SemaphoreType.DMA((2,)),
            pltpu.SemaphoreType.DMA((2,)),
            pltpu.SemaphoreType.DMA((1,)),
            pltpu.SemaphoreType.DMA((1,)),
        ],
        compiler_params=pltpu.CompilerParams(
            collective_id=0, has_side_effects=True, vmem_limit_bytes=48 * 2**20),
        name="wave_window",
    )(*[pltpu.with_memory_space_constraint(a, pltpu.HBM) for a in (
        spectrum.reshape(cells, SUB, lats), wind, land_sea, band_rows.reshape(1, lats))])
    parts = 4
    after, ocean = pl.pallas_call(
        functools.partial(finish_kernel, n, parts),
        out_shape=(jax.ShapeDtypeStruct((cells * SUB, lats), f32),
                   jax.ShapeDtypeStruct((4, band, columns * n), f32)),
        in_specs=[vmem, vmem],
        out_specs=(anywhere, anywhere),
        scratch_shapes=[pltpu.VMEM((4, band, columns * n), f32), pltpu.SemaphoreType.DMA((parts + 1,))],
        compiler_params=pltpu.CompilerParams(vmem_limit_bytes=2**20),
        name="hand_over",
    )(after, recv)
    return after.reshape(spectrum.shape), ocean


def solution(mesh):
    placed = (
        P(None, None, ("member", "gx"), None),
        P(None, ("member", "gx"), None),
        P("gx", None),
        P(),
    )
    return jax.shard_map(
        functools.partial(per_device, mesh.shape["gx"]),
        mesh=mesh,
        in_specs=placed,
        out_specs=(P(None, None, ("member", "gx"), None), P(None, "gx", "member")),
        check_vma=False,
    )
```

```python
import functools
import math

import jax
import jax.numpy as jnp
from jax import lax
from jax.experimental import pallas as pl
from jax.experimental.pallas import tpu as pltpu
from jax.sharding import PartitionSpec as P

STEPS = 3
SUB = 8
LEFT, RIGHT = 8, 10


def kernel(n, dirs, groups, spec, wind_in, land_in, bands_in, out, recv,
           trig, freq, wind, land, bands, x_ref, w_ref, g_ref, send, halo, wind_h, land_h,
           wind_b, mask_b, r_ref, drift_ref, e_send, e_halo, pick_t, sends, coef, table, grow_h,
           in_sem, small_sem, col_sem, meet, bulk_s, bulk_r, small_s, small_r, e_s, e_r, a_s, a_r):
    me = lax.axis_index("gx")
    right, left = lax.rem(me + 1, n), lax.rem(me + n - 1, n)
    late = lax.rem((me + 1) // 2, 2) == 0

    def greet(semaphore, reach):
        for peer in (lax.rem(me + reach, n), lax.rem(me + n - reach, n)):
            pl.semaphore_signal(semaphore, inc=1, device_id={"gx": peer},
                                device_id_type=pl.DeviceIdType.MESH)

    barrier = pltpu.get_barrier_semaphore()
    greet(barrier, 1)
    reaches = [2 ** i for i in range((n // 2 - 1).bit_length())]
    quarter = dirs // 4
    qbins = quarter * groups * SUB
    cells = dirs * groups * SUB
    lane = lax.broadcasted_iota(jnp.int32, (SUB, 128), 1)
    x_rows = x_ref.reshape(cells * SUB, 128)

    in_copy = pltpu.make_async_copy(spec, x_ref, in_sem.at[0])

    def column_copies(k, side):
        column = k if side else SUB - 1 - k
        return [pltpu.make_async_copy(
            spec.at[pl.ds(first * qbins, qbins), column],
            send.at[k, side, pl.ds(j * qbins, qbins)], col_sem.at[2 * k + side])
            for j, first in enumerate([(0, 3), (1, 2)][side])]

    def column_here(k, side):
        pltpu.make_async_copy(send.at[k, side], halo.at[k, side], col_sem.at[2 * k + side]).wait()

    tables_in = [pltpu.make_async_copy(src, dst, small_sem.at[i]) for i, (src, dst) in enumerate(
        [(wind_in, wind), (land_in, land), (bands_in, bands)])]
    columns_in = [[column_copies(k, side) for side in range(2)] for k in range(3)]
    odd = lax.rem(me, 2)
    for parity in range(2):
        @pl.when(odd == parity)
        def _(parity=parity):
            for copy in tables_in[:2] + columns_in[0][1 - parity] + columns_in[0][parity]:
                copy.start()
    tables_in[2].start()
    in_copy.start()
    for copy in sum(columns_in[1] + columns_in[2], []):
        copy.start()

    for d in range(dirs):
        angle = (d + 0.5) * (2.0 * math.pi / dirs)
        trig[0, d] = jnp.float32(math.cos(angle))
        trig[1, d] = jnp.float32(math.sin(angle))
    freqs = groups * SUB
    for f in range(groups):
        level = (lax.broadcasted_iota(jnp.int32, (SUB, 128), 0) + f * SUB).astype(jnp.float32)
        weight = (level + 1.0) * (1.0 / freqs)
        grown = jnp.exp(level * math.log(1.1))
        freq[0, f] = 0.45 / grown
        freq[1, f] = grown * (2.0 * math.pi * 0.0418 / 9.81)
        freq[2, f] = 0.3 * weight * weight
        freq[3, f] = weight * (3.0 / math.sqrt(dirs * freqs))

    def remote(src, dst, send_sem, recv_sem, target):
        return pltpu.make_async_remote_copy(
            src_ref=src, dst_ref=dst, send_sem=send_sem, recv_sem=recv_sem,
            device_id={"gx": target}, device_id_type=pl.DeviceIdType.MESH)

    def arrived(ref, sem):
        pltpu.make_async_copy(ref, ref, sem).wait()

    bulk = [[remote(send.at[k, side], halo.at[k, side], bulk_s.at[0],
                    bulk_r.at[k + side * (k // 2)],
                    (right, left)[side]) for side in range(2)] for k in range(3)]
    ends = (pl.ds(SUB - 2, 2), pl.ds(0, 2))
    small = [remote(src, dst, small_s.at[j], small_r.at[j], (right, left)[side])
             for side in range(2) for j, (src, dst) in enumerate([
                 (wind.at[:, ends[side]], wind_h.at[side, :, ends[side]]),
                 (land.at[ends[side]], land_h.at[side, ends[side]])])]
    energy_msg = [[remote(e_send.at[s, ends[side]], e_halo.at[s, side, ends[side]], e_s.at[s],
                          e_r.at[s + side * s], (right, left)[side]) for side in range(2)] for s in range(2)]
    wind_rows, land_rows = wind_h.at[:, :, ends[1]], land_h.at[:, ends[1]]

    column_here(0, 1 - odd)
    pl.semaphore_wait(barrier, 2)
    for copy in tables_in:
        copy.wait()
    for copy in small:
        copy.start()

    def first_column(side):
        remote(send.at[0, side], halo.at[0, side], bulk_s.at[0], bulk_r.at[0],
               jnp.where(side == 0, right, left)).start()

    first_column(1 - odd)
    column_here(0, odd)
    first_column(odd)
    if reaches:
        greet(meet.at[0], reaches[0])

    def spread(slot, wind_tile, land_tile, column):
        for c in range(2):
            wind_b[c, slot] = jnp.broadcast_to(wind_tile[c][column:column + 1], (SUB, 128))
        mask_b[slot] = jnp.broadcast_to(
            land_tile[column:column + 1].astype(jnp.float32), (SUB, 128))

    own_wind = [wind[0], wind[1]]
    own_land = land[...]
    for x in range(SUB):
        spread(x, own_wind, own_land, x)

    for k in (1, 2):
        for side in range(2):
            column_here(k, side)

    def launch(k, when):
        @pl.when(when)
        def _():
            for copy in bulk[k]:
                copy.start()

    def spread_word(rounds):
        for i in rounds:
            pl.semaphore_wait(meet.at[i], 2)
            if i + 1 < len(reaches):
                greet(meet.at[i + 1], reaches[i + 1])

    for copy in bulk[1]:
        copy.start()
    in_copy.wait()

    def scalars(d):
        return trig[0, d], trig[1, d]

    halves = [(0, 2 * quarter, True), (quarter, 0, False)]

    def coefficients(cosine, sine, f, east, turn):
        k = freq[0, f]
        along_x = k * (cosine if east else -cosine)
        along_y = k * jnp.abs(sine)
        centre = 1.0 - along_x - along_y
        return centre, along_x, jnp.where(lane == 127 * turn, 0.0, along_y)

    def stencil(bin_tile):
        return table[0, bin_tile], table[1, bin_tile], table[2, bin_tile]

    def shifted(value, turn):
        return pltpu.roll(value, 1 + 126 * turn, 1)

    def growth_of(cosine, sine, f, slot):
        ratio = (wind_b[0, slot] * cosine + wind_b[1, slot] * sine) * freq[1, f]
        return 0.05 * jnp.minimum(jnp.maximum(ratio - 1.0, 0.0), 4.0)

    zero = jnp.zeros((SUB, 128), jnp.float32)

    def main(step, sums):
        for d0, skip, east in halves:
            def body(i, sums, d0=d0, skip=skip, east=east):
                turn = i // quarter
                d = d0 + i + skip * turn
                sums = list(sums)
                if step == 0:
                    cosine, sine = scalars(d)
                    speed = [wind_b[0, x] * cosine + wind_b[1, x] * sine for x in range(SUB)]
                for f in range(groups):
                    if step == 0:
                        centre, along_x, along_y = coefficients(cosine, sine, f, east, turn)
                        for c, value in enumerate((centre, along_x, along_y)):
                            table[c, d * groups + f] = value
                    else:
                        centre, along_x, along_y = stencil(d * groups + f)
                    before = None
                    for x in (range(SUB) if east else range(SUB - 1, -1, -1)):
                        at = (d * groups + f) * SUB + x
                        if step == 0:
                            value = x_rows[pl.ds((d * groups + f) * SUB * SUB + x, SUB, stride=SUB), :]
                            g_ref[at] = 1.0 + 0.05 * jnp.minimum(
                                jnp.maximum(speed[x] * freq[1, f] - 1.0, 0.0), 4.0)
                        else:
                            value = w_ref[at] * g_ref[at] * r_ref[x, f]
                        new = centre * value + along_y * shifted(value, turn)
                        if before is not None:
                            new = new + along_x * before
                        before = value
                        w_ref[at] = new
                        sums[x] = sums[x] + new
                return tuple(sums)

            sums = lax.fori_loop(0, 2 * quarter, body, tuple(sums), unroll=9)
        return sums

    def edges():
        for side, (d0, skip, east) in enumerate(halves):
            yield side, d0, skip, east, (LEFT if east else RIGHT), (0 if east else SUB - 1)

    def over_tiles(body, carry, unroll=3):
        return lax.fori_loop(0, 2 * quarter, body, carry, unroll=unroll)

    def grow_halo():
        for side, d0, skip, east, slot, edge in edges():
            def body(i, carry, d0=d0, skip=skip, side=side, slot=slot):
                d = d0 + i + skip * (i // quarter)
                cosine, sine = scalars(d)
                for f in range(groups):
                    for depth in range(2):
                        grow_h[side, depth, pl.ds((i * groups + f) * SUB, SUB), :] = (
                            1.0 + growth_of(cosine, sine, f, slot + depth))
                return carry

            over_tiles(body, 0)

    def prepare(step):
        for side, d0, skip, east, slot, edge in edges():
            def body(i, carry, d0=d0, skip=skip, east=east, side=side, slot=slot):
                turn = i // quarter
                d = d0 + i + skip * turn
                for f in range(groups):
                    centre, along_x, along_y = stencil(d * groups + f)
                    at = pl.ds((i * groups + f) * SUB, SUB)

                    def local(k, depth):
                        value = halo[k, side, at, :]
                        grown = grow_h[side, depth, at, :]
                        return (centre * value + along_y * shifted(value, turn)), grown

                    near, grown = local(0, 0)
                    if step == 1:
                        halo[0, side, at, :] = near * grown
                        coef[side, at, :] = along_x * grown
                    else:
                        far, grown_far = local(1, 1)
                        grown = along_x * grown
                        reach = along_x * grown_far * r_ref[slot + 1, f]
                        halo[0, side, at, :] = grown * (near + reach * far)
                        coef[side, at, :] = grown * reach * along_x
                return carry

            over_tiles(body, 0, 6)

    def contribute(acc, d, moved, grown):
        cosine, sine = scalars(d)
        acc = list(acc)
        flux = zero
        for f in range(groups):
            flux = flux + freq[3, f] * (grown[f] - moved[f])
            acc[2 + f] = acc[2 + f] + cosine * grown[f]
            acc[2 + groups + f] = acc[2 + groups + f] + sine * grown[f]
        acc[0] = acc[0] + cosine * flux
        acc[1] = acc[1] + sine * flux
        return acc

    def fix(step, sums):
        totals = {}
        for side, d0, skip, east, slot, edge in edges():
            def body(i, total, d0=d0, skip=skip, side=side, slot=slot, edge=edge):
                d = d0 + i + skip * (i // quarter)
                for f in range(groups):
                    at = pl.ds((i * groups + f) * SUB, SUB)
                    flow = halo[0, side, at, :]
                    if step == 1:
                        flow = r_ref[slot, f] * (flow + coef[side, at, :] * halo[1, side, at, :])
                        halo[0, side, at, :] = flow
                    extra = table[1, d * groups + f] * flow
                    cell = (d * groups + f) * SUB + edge
                    w_ref[cell] = w_ref[cell] + extra
                    total = total + extra
                return total

            totals[edge] = over_tiles(body, sums[edge], 6)
        return tuple(totals.get(x, sums[x]) for x in range(SUB))

    def energy_rows(sums, which):
        return [jnp.sum(sums[x] * mask_b[x], axis=0, keepdims=True) for x in which]

    def energy_tile(sums):
        return jnp.concatenate(energy_rows(sums, range(SUB)), axis=0) * (1.0 / cells)

    def factor(tile, column, mask_slot, slot):
        ratio = jnp.broadcast_to(tile[column:column + 1], (SUB, 128))
        for f in range(groups):
            r_ref[slot, f] = mask_b[mask_slot] / (1.0 + freq[2, f] * ratio)

    def own_factors(tile):
        ratio = tile / (0.5 + tile)
        for x in range(SUB):
            factor(ratio, x, x, x)

    inner, outer = list(range(1, SUB - 1)), [0, SUB - 1]

    def last_factors(which, sums):
        for x, row in zip(which, energy_rows(sums, which)):
            tile = row * (1.0 / cells)
            ratio = jnp.broadcast_to(tile / (0.5 + tile), (SUB, 128))
            for f in range(groups):
                r_ref[x, f] = mask_b[x] / (1.0 + freq[2, f] * ratio)

    def row_sums(which, values):
        rows_of = {}
        for c in range(4):
            for j, x in enumerate(which):
                value = values[c * len(which) + j]
                if c < 2:
                    value = value * mask_b[x]
                rows_of[c * SUB + x] = jnp.sum(value, axis=0, keepdims=True)
        return rows_of

    def gathered_outer():
        size = 2 + 2 * groups

        def gather(d, carry):
            done = []
            for j, x in enumerate(outer):
                cells_of = [(d * groups + f) * SUB + x for f in range(groups)]
                moved = [w_ref[at] for at in cells_of]
                grown = [g_ref[at] * value for at, value in zip(cells_of, moved)]
                done += contribute(carry[j * size:(j + 1) * size], d, moved, grown)
            return tuple(done)

        total = lax.fori_loop(0, dirs, gather, (zero,) * (2 * size), unroll=2)
        return {x: total[j * size:(j + 1) * size] for j, x in enumerate(outer)}

    def gathered(which, sums):
        last_factors(which, sums)
        for x in which:
            for f in range(groups):
                drift_ref[x, f] = freq[3, f] * r_ref[x, f]

        def gather(d, carry):
            cosine, sine = scalars(d)
            carry = list(carry)
            m = len(which)
            for j, x in enumerate(which):
                flux, drift = zero, zero
                for f in range(groups):
                    at = (d * groups + f) * SUB + x
                    moved = w_ref[at]
                    grown = g_ref[at] * moved
                    flux = flux + freq[3, f] * (grown - moved)
                    drift = drift + drift_ref[x, f] * grown
                carry[j] = carry[j] + cosine * flux
                carry[m + j] = carry[m + j] + sine * flux
                carry[2 * m + j] = carry[2 * m + j] + cosine * drift
                carry[3 * m + j] = carry[3 * m + j] + sine * drift
            return tuple(carry)

        return row_sums(which, lax.fori_loop(
            0, dirs, gather, (zero,) * (4 * len(which)), unroll=2))

    lat = lax.broadcasted_iota(jnp.int32, (128, 128), 0)
    pick_t[...] = (lat == bands[...]).astype(jnp.float32).T
    sums = main(0, (zero,) * SUB)
    spread_word(range(0, 1) if reaches else [])
    arrived(wind_rows, small_r.at[0])
    arrived(land_rows, small_r.at[1])
    for side in range(2):
        tiles = [wind_h[side, 0], wind_h[side, 1]]
        land_tile = land_h[side]
        for depth in range(2):
            spread((LEFT if side == 0 else RIGHT) + depth, tiles, land_tile,
                   SUB - 1 - depth if side == 0 else depth)
    grow_halo()
    arrived(halo.at[0], bulk_r.at[0])
    sums = fix(0, sums)
    for step in (1, 2):
        tile = energy_tile(sums)
        e_send[step - 1] = tile
        own_factors(tile)
        for copy in energy_msg[step - 1]:
            copy.start()
        launch(2, late if step == 2 else jnp.logical_not(late))
        sums = main(step, (zero,) * SUB)
        if step == 1:
            spread_word(range(1, min(2, len(reaches))))
        else:
            spread_word(range(2, len(reaches)))
        prepare(step)
        if step == 2:
            inner_rows = gathered(inner, sums)
            outer_parts = gathered_outer()
        if step == 2:
            break
        arrived(halo.at[1], bulk_r.at[1])
        arrived(e_halo.at[0, :, ends[1]], e_r.at[0])
        for side in range(2):
            seen = e_halo[0, side]
            ratio = seen / (0.5 + seen)
            base = LEFT if side == 0 else RIGHT
            for depth in range(2):
                factor(ratio, SUB - 1 - depth if side == 0 else depth, base + depth, base + depth)
        sums = fix(1, sums)

    def by_side(first, second):
        return [jnp.where(odd == 1, a, b) for a, b in zip(first, second)]

    def last_fix(side, start):
        arrived(halo.at[2, side], bulk_r.at[2 + side])
        arrived(e_halo.at[1, side, ends[1]], e_r.at[1 + side])
        slot, edge = LEFT + side * (RIGHT - LEFT), side * (SUB - 1)
        seen = e_halo[1, side, pl.ds((1 - side) * (SUB - 1), 1), :]
        ratio = jnp.broadcast_to(seen / (0.5 + seen), (SUB, 128))
        scale = [mask_b[slot] / (1.0 + freq[2, f] * ratio) for f in range(groups)]
        for f in range(groups):
            r_ref[slot + 4, f] = scale[f]

        def body(i, carry):
            total, acc = carry[0], carry[1:]
            d = side * quarter + i + (1 - side) * 2 * quarter * (i // quarter)
            moved, grown = [], []
            for f in range(groups):
                at = pl.ds((i * groups + f) * SUB, SUB)
                cell = (d * groups + f) * SUB + edge
                extra = r_ref[slot + 4, f] * (
                    halo[0, side, at, :] + coef[side, at, :] * halo[2, side, at, :])
                w_ref[cell] = w_ref[cell] + extra
                total = total + extra
                moved.append(extra)
                grown.append(g_ref[cell] * extra)
            return (total, *contribute(acc, d, moved, grown))

        return over_tiles(body, tuple(start), 6)

    west_edge = (sums[0], *outer_parts[0])
    east_edge = (sums[SUB - 1], *outer_parts[SUB - 1])
    near = last_fix(1 - odd, by_side(west_edge, east_edge))
    far = last_fix(odd, by_side(east_edge, west_edge))
    west_edge, east_edge = by_side(near, far), by_side(far, near)
    sums = (west_edge[0],) + tuple(sums[1:-1]) + (east_edge[0],)
    outer_parts = {0: west_edge[1:], SUB - 1: east_edge[1:]}

    last_factors(outer, sums)
    values = [None] * 8
    for j, x in enumerate(outer):
        part = outer_parts[x]
        values[j], values[2 + j] = part[0], part[1]
        for c in range(2):
            drift = zero
            for f in range(groups):
                drift = drift + (freq[3, f] * r_ref[x, f]) * part[2 + c * groups + f]
            values[4 + 2 * c + j] = drift
    all_rows = {**inner_rows, **row_sums(outer, values)}
    total = [all_rows[j] for j in range(4 * SUB)]
    total.append(jnp.zeros((128 - 4 * SUB, 128), jnp.float32))
    stacked = jnp.concatenate(total, axis=0)
    picked = lax.dot_general(
        pick_t[...], stacked, (((1,), (1,)), ((), ())), precision=lax.Precision.HIGHEST,
        preferred_element_type=jnp.float32)
    band = 128 // n
    for k in range(n):
        sends[k] = picked[k * band:(k + 1) * band]

    def begin(i, _):
        step = (i // 2) * (1 - 2 * lax.rem(i, 2))
        target = lax.rem(me + n // 2 + step + n, n)
        remote(sends.at[target], recv.at[me], a_s.at[0], a_r.at[0], target).start()
        return 0

    lax.fori_loop(1, n, begin, 0, unroll=3)
    recv[pl.ds(me, 1)] = sends[pl.ds(me, 1)]

    def write(d, _):
        for f in range(groups):
            for x in range(SUB):
                at = (d * groups + f) * SUB + x
                moved = w_ref[at]
                out[pl.ds((d * groups + f) * SUB * SUB + x, SUB, stride=SUB), :] = (
                    moved * g_ref[at] * r_ref[x, f])
        return 0

    lax.fori_loop(0, dirs, write, 0, unroll=2)
    arrived(send, bulk_s.at[0])
    arrived(wind_rows, small_s.at[0])
    arrived(land_rows, small_s.at[1])
    for s in range(2):
        arrived(e_halo.at[s, :, ends[1]], e_s.at[s])
    others = sends.at[pl.ds(0, n - 1)]
    arrived(others, a_s.at[0])
    arrived(others, a_r.at[0])


def finish_kernel(n, parts, out, recv, after, ocean_out, ocean, sem):
    rows = out.shape[0] // parts
    copies = []
    for q in range(parts):
        part = pl.ds(q * rows, rows)
        copies.append(pltpu.make_async_copy(out.at[part], after.at[part], sem.at[q]))
        copies[-1].start()
    band = 128 // n
    per_tile = 128 // SUB
    block = lax.broadcasted_iota(jnp.int32, (band, 128), 1) // SUB
    for tile in range(max(1, n // per_tile)):
        for c in range(4):
            built = jnp.zeros((band, 128), jnp.float32)
            for k in range(min(n, per_tile)):
                moved = pltpu.roll(recv[tile * per_tile + k], (SUB * (k - c)) % 128, 1)
                built = jnp.where(block == k, moved, built)
            ocean[c, :, tile * 128:(tile + 1) * 128] = built
    copies.append(pltpu.make_async_copy(ocean, ocean_out, sem.at[parts]))
    copies[-1].start()
    for copy in copies:
        copy.wait()


def per_device(n, spectrum, wind, land_sea, band_rows):
    dirs, freqs, columns, lats = spectrum.shape
    groups = freqs // SUB
    half = dirs // 2 * groups * SUB
    band = lats // n
    f32 = jnp.float32
    anywhere = pl.BlockSpec(memory_space=pltpu.HBM)
    vmem = pl.BlockSpec(memory_space=pltpu.VMEM)
    cells = dirs * groups * SUB
    after, recv = pl.pallas_call(
        functools.partial(kernel, n, dirs, groups),
        out_shape=(pltpu.VMEM((cells * SUB, lats), f32), pltpu.VMEM((n, band, 128), f32)),
        in_specs=[anywhere] * 4,
        out_specs=(vmem, vmem),
        scratch_shapes=[
            pltpu.SMEM((2, dirs), f32),
            pltpu.VMEM((4, groups, SUB, lats), f32),
            pltpu.VMEM((2, SUB, lats), f32),
            pltpu.VMEM((SUB, lats), jnp.int32),
            pltpu.VMEM((1, lats), jnp.int32),
            pltpu.VMEM((cells, SUB, lats), f32),
            pltpu.VMEM((cells, SUB, lats), f32),
            pltpu.VMEM((cells, SUB, lats), f32),
            pltpu.VMEM((3, 2, half, lats), f32),
            pltpu.VMEM((3, 2, half, lats), f32),
            pltpu.VMEM((2, 2, SUB, lats), f32),
            pltpu.VMEM((2, SUB, lats), jnp.int32),
            pltpu.VMEM((2, 12, SUB, lats), f32),
            pltpu.VMEM((12, SUB, lats), f32),
            pltpu.VMEM((16, groups, SUB, lats), f32),
            pltpu.VMEM((SUB, groups, SUB, lats), f32),
            pltpu.VMEM((2, SUB, lats), f32),
            pltpu.VMEM((2, 2, SUB, lats), f32),
            pltpu.VMEM((128, 128), f32),
            pltpu.VMEM((n, band, 128), f32),
            pltpu.VMEM((2, half, lats), f32),
            pltpu.VMEM((3, dirs * groups, SUB, lats), f32),
            pltpu.VMEM((2, 2, half, lats), f32),
            pltpu.SemaphoreType.DMA((1,)),
            pltpu.SemaphoreType.DMA((3,)),
            pltpu.SemaphoreType.DMA((6,)),
            pltpu.SemaphoreType.REGULAR((max(1, (n // 2 - 1).bit_length()),)),
            pltpu.SemaphoreType.DMA((1,)),
            pltpu.SemaphoreType.DMA((4,)),
            pltpu.SemaphoreType.DMA((2,)),
            pltpu.SemaphoreType.DMA((2,)),
            pltpu.SemaphoreType.DMA((2,)),
            pltpu.SemaphoreType.DMA((3,)),
            pltpu.SemaphoreType.DMA((1,)),
            pltpu.SemaphoreType.DMA((1,)),
        ],
        compiler_params=pltpu.CompilerParams(
            collective_id=0, has_side_effects=True, vmem_limit_bytes=48 * 2**20),
        name="wave_window",
    )(*[pltpu.with_memory_space_constraint(a, pltpu.HBM) for a in (
        spectrum.reshape(cells, SUB, lats), wind, land_sea, band_rows.reshape(1, lats))])
    parts = 1
    after, ocean = pl.pallas_call(
        functools.partial(finish_kernel, n, parts),
        out_shape=(jax.ShapeDtypeStruct((cells * SUB, lats), f32),
                   jax.ShapeDtypeStruct((4, band, columns * n), f32)),
        in_specs=[vmem, vmem],
        out_specs=(anywhere, anywhere),
        scratch_shapes=[pltpu.VMEM((4, band, columns * n), f32), pltpu.SemaphoreType.DMA((parts + 1,))],
        compiler_params=pltpu.CompilerParams(vmem_limit_bytes=2**20),
        name="hand_over",
    )(after, recv)
    return after.reshape(spectrum.shape), ocean


def solution(mesh):
    placed = (
        P(None, None, ("member", "gx"), None),
        P(None, ("member", "gx"), None),
        P("gx", None),
        P(),
    )
    return jax.shard_map(
        functools.partial(per_device, mesh.shape["gx"]),
        mesh=mesh,
        in_specs=placed,
        out_specs=(P(None, None, ("member", "gx"), None), P(None, "gx", "member")),
        check_vma=False,
    )
```

```python
import functools
import math

import jax
import jax.numpy as jnp
from jax import lax
from jax.experimental import pallas as pl
from jax.experimental.pallas import tpu as pltpu
from jax.sharding import PartitionSpec as P

STEPS = 3
SUB = 8
LEFT, RIGHT = 8, 10


def packing(n):
    pack = min(4, 128 // n)
    return pack, 128 // pack


def kernel(n, dirs, groups, spec, wind_in, land_in, bands_in, out, recv,
           trig, freq, wind, land, bands, x_ref, w_ref, g_ref, send, halo, wind_h, land_h,
           wind_b, mask_b, r_ref, drift_ref, e_send, e_halo, pick_t, sends, coef, table, grow_h,
           in_sem, small_sem, col_sem, meet, bulk_s, bulk_r, small_s, small_r, e_s, e_r, a_s, a_r):
    me = lax.axis_index("gx")
    right, left = lax.rem(me + 1, n), lax.rem(me + n - 1, n)
    late = lax.rem((me + 1) // 2, 2) == 0

    def greet(semaphore, reach):
        for peer in (lax.rem(me + reach, n), lax.rem(me + n - reach, n)):
            pl.semaphore_signal(semaphore, inc=1, device_id={"gx": peer},
                                device_id_type=pl.DeviceIdType.MESH)

    barrier = pltpu.get_barrier_semaphore()
    greet(barrier, 1)
    reaches = [2 ** i for i in range((n // 2 - 1).bit_length())]
    quarter = dirs // 4
    qbins = quarter * groups * SUB
    cells = dirs * groups * SUB
    lane = lax.broadcasted_iota(jnp.int32, (SUB, 128), 1)
    x_rows = x_ref.reshape(cells * SUB, 128)

    in_copy = pltpu.make_async_copy(spec, x_ref, in_sem.at[0])

    def column_copies(k):
        return [pltpu.make_async_copy(
            spec.at[pl.ds(first, bins), column], send.at[k, side, pl.ds(to, bins)], col_sem.at[k])
            for first, bins, side, to, column in [
                (0, qbins, 0, 0, SUB - 1 - k), (3 * qbins, qbins, 0, qbins, SUB - 1 - k),
                (qbins, 2 * qbins, 1, 0, k)]]

    def columns_here(k):
        pltpu.make_async_copy(send.at[k], halo.at[k], col_sem.at[k]).wait()

    tables_in = [pltpu.make_async_copy(src, dst, small_sem.at[i]) for i, (src, dst) in enumerate(
        [(wind_in, wind), (land_in, land), (bands_in, bands)])]
    columns_in = [column_copies(k) for k in range(3)]
    for copy in columns_in[0] + tables_in:
        copy.start()
    in_copy.start()
    for copy in columns_in[1] + columns_in[2]:
        copy.start()

    for d in range(dirs):
        angle = (d + 0.5) * (2.0 * math.pi / dirs)
        trig[0, d] = jnp.float32(math.cos(angle))
        trig[1, d] = jnp.float32(math.sin(angle))
    freqs = groups * SUB
    for f in range(groups):
        level = (lax.broadcasted_iota(jnp.int32, (SUB, 128), 0) + f * SUB).astype(jnp.float32)
        weight = (level + 1.0) * (1.0 / freqs)
        grown = jnp.exp(level * math.log(1.1))
        freq[0, f] = 0.45 / grown
        freq[1, f] = grown * (2.0 * math.pi * 0.0418 / 9.81)
        freq[2, f] = 0.3 * weight * weight
        freq[3, f] = weight * (3.0 / math.sqrt(dirs * freqs))

    def remote(src, dst, send_sem, recv_sem, target):
        return pltpu.make_async_remote_copy(
            src_ref=src, dst_ref=dst, send_sem=send_sem, recv_sem=recv_sem,
            device_id={"gx": target}, device_id_type=pl.DeviceIdType.MESH)

    def arrived(ref, sem):
        pltpu.make_async_copy(ref, ref, sem).wait()

    bulk = [[remote(send.at[k, side], halo.at[k, side], bulk_s.at[0],
                    bulk_r.at[k + side * (k // 2)],
                    (right, left)[side]) for side in range(2)] for k in range(3)]
    ends = (pl.ds(SUB - 2, 2), pl.ds(0, 2))
    small = [remote(src, dst, small_s.at[j], small_r.at[j], (right, left)[side])
             for side in range(2) for j, (src, dst) in enumerate([
                 (wind.at[:, ends[side]], wind_h.at[side, :, ends[side]]),
                 (land.at[ends[side]], land_h.at[side, ends[side]])])]
    energy_msg = [[remote(e_send.at[s, ends[side]], e_halo.at[s, side, ends[side]], e_s.at[s],
                          e_r.at[s + side * s], (right, left)[side]) for side in range(2)] for s in range(2)]
    wind_rows, land_rows = wind_h.at[:, :, ends[1]], land_h.at[:, ends[1]]

    columns_here(0)
    pl.semaphore_wait(barrier, 2)
    for copy in tables_in:
        copy.wait()
    for copy in small + bulk[0]:
        copy.start()
    if reaches:
        greet(meet.at[0], reaches[0])

    def spread(slot, wind_tile, land_tile, column):
        for c in range(2):
            wind_b[c, slot] = jnp.broadcast_to(wind_tile[c][column:column + 1], (SUB, 128))
        mask_b[slot] = jnp.broadcast_to(
            land_tile[column:column + 1].astype(jnp.float32), (SUB, 128))

    own_wind = [wind[0], wind[1]]
    own_land = land[...]
    for x in range(SUB):
        spread(x, own_wind, own_land, x)

    columns_here(1)
    columns_here(2)

    def launch(k, when):
        @pl.when(when)
        def _():
            for copy in bulk[k]:
                copy.start()

    def spread_word(rounds):
        for i in rounds:
            pl.semaphore_wait(meet.at[i], 2)
            if i + 1 < len(reaches):
                greet(meet.at[i + 1], reaches[i + 1])

    for copy in bulk[1]:
        copy.start()
    in_copy.wait()

    def scalars(d):
        return trig[0, d], trig[1, d]

    halves = [(0, 2 * quarter, True), (quarter, 0, False)]

    def coefficients(cosine, sine, f, east, turn):
        k = freq[0, f]
        along_x = k * (cosine if east else -cosine)
        along_y = k * jnp.abs(sine)
        centre = 1.0 - along_x - along_y
        return centre, along_x, jnp.where(lane == 127 * turn, 0.0, along_y)

    def stencil(bin_tile):
        return table[0, bin_tile], table[1, bin_tile], table[2, bin_tile]

    def shifted(value, turn):
        return pltpu.roll(value, 1 + 126 * turn, 1)

    def growth_of(cosine, sine, f, slot):
        ratio = (wind_b[0, slot] * cosine + wind_b[1, slot] * sine) * freq[1, f]
        return 0.05 * jnp.minimum(jnp.maximum(ratio - 1.0, 0.0), 4.0)

    zero = jnp.zeros((SUB, 128), jnp.float32)

    def main(step, sums):
        for d0, skip, east in halves:
            def body(i, sums, d0=d0, skip=skip, east=east):
                turn = i // quarter
                d = d0 + i + skip * turn
                sums = list(sums)
                if step == 0:
                    cosine, sine = scalars(d)
                    speed = [wind_b[0, x] * cosine + wind_b[1, x] * sine for x in range(SUB)]
                for f in range(groups):
                    if step == 0:
                        centre, along_x, along_y = coefficients(cosine, sine, f, east, turn)
                        for c, value in enumerate((centre, along_x, along_y)):
                            table[c, d * groups + f] = value
                    else:
                        centre, along_x, along_y = stencil(d * groups + f)
                    before = None
                    for x in (range(SUB) if east else range(SUB - 1, -1, -1)):
                        at = (d * groups + f) * SUB + x
                        if step == 0:
                            value = x_rows[pl.ds((d * groups + f) * SUB * SUB + x, SUB, stride=SUB), :]
                            g_ref[at] = 1.0 + 0.05 * jnp.minimum(
                                jnp.maximum(speed[x] * freq[1, f] - 1.0, 0.0), 4.0)
                        else:
                            value = w_ref[at] * g_ref[at] * r_ref[x, f]
                        new = centre * value + along_y * shifted(value, turn)
                        if before is not None:
                            new = new + along_x * before
                        before = value
                        w_ref[at] = new
                        sums[x] = sums[x] + new
                return tuple(sums)

            sums = lax.fori_loop(0, 2 * quarter, body, tuple(sums), unroll=9)
        return sums

    def edges():
        for side, (d0, skip, east) in enumerate(halves):
            yield side, d0, skip, east, (LEFT if east else RIGHT), (0 if east else SUB - 1)

    def over_tiles(body, carry, unroll=3):
        return lax.fori_loop(0, 2 * quarter, body, carry, unroll=unroll)

    def grow_halo():
        for side, d0, skip, east, slot, edge in edges():
            def body(i, carry, d0=d0, skip=skip, side=side, slot=slot):
                d = d0 + i + skip * (i // quarter)
                cosine, sine = scalars(d)
                for f in range(groups):
                    for depth in range(2):
                        grow_h[side, depth, pl.ds((i * groups + f) * SUB, SUB), :] = (
                            1.0 + growth_of(cosine, sine, f, slot + depth))
                return carry

            over_tiles(body, 0)

    def prepare(step):
        for side, d0, skip, east, slot, edge in edges():
            def body(i, carry, d0=d0, skip=skip, east=east, side=side, slot=slot):
                turn = i // quarter
                d = d0 + i + skip * turn
                for f in range(groups):
                    centre, along_x, along_y = stencil(d * groups + f)
                    at = pl.ds((i * groups + f) * SUB, SUB)

                    def local(k, depth):
                        value = halo[k, side, at, :]
                        grown = grow_h[side, depth, at, :]
                        return (centre * value + along_y * shifted(value, turn)), grown

                    near, grown = local(0, 0)
                    if step == 1:
                        halo[0, side, at, :] = near * grown
                        coef[side, at, :] = along_x * grown
                    else:
                        far, grown_far = local(1, 1)
                        grown = along_x * grown
                        reach = along_x * grown_far * r_ref[slot + 1, f]
                        halo[0, side, at, :] = grown * (near + reach * far)
                        coef[side, at, :] = grown * reach * along_x
                return carry

            over_tiles(body, 0, 6)

    def contribute(acc, d, moved, grown):
        cosine, sine = scalars(d)
        acc = list(acc)
        flux = zero
        for f in range(groups):
            flux = flux + freq[3, f] * (grown[f] - moved[f])
            acc[2 + f] = acc[2 + f] + cosine * grown[f]
            acc[2 + groups + f] = acc[2 + groups + f] + sine * grown[f]
        acc[0] = acc[0] + cosine * flux
        acc[1] = acc[1] + sine * flux
        return acc

    def fix(step, sums):
        totals = {}
        for side, d0, skip, east, slot, edge in edges():
            def body(i, total, d0=d0, skip=skip, side=side, slot=slot, edge=edge):
                d = d0 + i + skip * (i // quarter)
                for f in range(groups):
                    at = pl.ds((i * groups + f) * SUB, SUB)
                    flow = halo[0, side, at, :]
                    if step == 1:
                        flow = r_ref[slot, f] * (flow + coef[side, at, :] * halo[1, side, at, :])
                        halo[0, side, at, :] = flow
                    extra = table[1, d * groups + f] * flow
                    cell = (d * groups + f) * SUB + edge
                    w_ref[cell] = w_ref[cell] + extra
                    total = total + extra
                return total

            totals[edge] = over_tiles(body, sums[edge], 6)
        return tuple(totals.get(x, sums[x]) for x in range(SUB))

    def energy_rows(sums, which):
        return [jnp.sum(sums[x] * mask_b[x], axis=0, keepdims=True) for x in which]

    def energy_tile(sums):
        return jnp.concatenate(energy_rows(sums, range(SUB)), axis=0) * (1.0 / cells)

    def factor(tile, column, mask_slot, slot):
        ratio = jnp.broadcast_to(tile[column:column + 1], (SUB, 128))
        for f in range(groups):
            r_ref[slot, f] = mask_b[mask_slot] / (1.0 + freq[2, f] * ratio)

    def own_factors(tile):
        ratio = tile / (0.5 + tile)
        for x in range(SUB):
            factor(ratio, x, x, x)

    inner, outer = list(range(1, SUB - 1)), [0, SUB - 1]

    def last_factors(which, sums):
        for x, row in zip(which, energy_rows(sums, which)):
            tile = row * (1.0 / cells)
            ratio = jnp.broadcast_to(tile / (0.5 + tile), (SUB, 128))
            for f in range(groups):
                r_ref[x, f] = mask_b[x] / (1.0 + freq[2, f] * ratio)

    def row_sums(which, values):
        rows_of = {}
        for c in range(4):
            for j, x in enumerate(which):
                value = values[c * len(which) + j]
                if c < 2:
                    value = value * mask_b[x]
                rows_of[c * SUB + x] = jnp.sum(value, axis=0, keepdims=True)
        return rows_of

    def gathered_outer():
        size = 2 + 2 * groups

        def gather(d, carry):
            done = []
            for j, x in enumerate(outer):
                cells_of = [(d * groups + f) * SUB + x for f in range(groups)]
                moved = [w_ref[at] for at in cells_of]
                grown = [g_ref[at] * value for at, value in zip(cells_of, moved)]
                done += contribute(carry[j * size:(j + 1) * size], d, moved, grown)
            return tuple(done)

        total = lax.fori_loop(0, dirs, gather, (zero,) * (2 * size), unroll=2)
        return {x: total[j * size:(j + 1) * size] for j, x in enumerate(outer)}

    def gathered(which, sums):
        last_factors(which, sums)
        for x in which:
            for f in range(groups):
                drift_ref[x, f] = freq[3, f] * r_ref[x, f]

        def gather(d, carry):
            cosine, sine = scalars(d)
            carry = list(carry)
            m = len(which)
            for j, x in enumerate(which):
                flux, drift = zero, zero
                for f in range(groups):
                    at = (d * groups + f) * SUB + x
                    moved = w_ref[at]
                    grown = g_ref[at] * moved
                    flux = flux + freq[3, f] * (grown - moved)
                    drift = drift + drift_ref[x, f] * grown
                carry[j] = carry[j] + cosine * flux
                carry[m + j] = carry[m + j] + sine * flux
                carry[2 * m + j] = carry[2 * m + j] + cosine * drift
                carry[3 * m + j] = carry[3 * m + j] + sine * drift
            return tuple(carry)

        return row_sums(which, lax.fori_loop(
            0, dirs, gather, (zero,) * (4 * len(which)), unroll=2))

    lat = lax.broadcasted_iota(jnp.int32, (128, 128), 0)
    pick_t[...] = (lat == bands[...]).astype(jnp.float32).T
    sums = main(0, (zero,) * SUB)
    spread_word(range(0, 1) if reaches else [])
    arrived(wind_rows, small_r.at[0])
    arrived(land_rows, small_r.at[1])
    for side in range(2):
        tiles = [wind_h[side, 0], wind_h[side, 1]]
        land_tile = land_h[side]
        for depth in range(2):
            spread((LEFT if side == 0 else RIGHT) + depth, tiles, land_tile,
                   SUB - 1 - depth if side == 0 else depth)
    grow_halo()
    arrived(halo.at[0], bulk_r.at[0])
    sums = fix(0, sums)
    for step in (1, 2):
        tile = energy_tile(sums)
        e_send[step - 1] = tile
        own_factors(tile)
        for copy in energy_msg[step - 1]:
            copy.start()
        launch(2, late if step == 2 else jnp.logical_not(late))
        sums = main(step, (zero,) * SUB)
        if step == 1:
            spread_word(range(1, min(2, len(reaches))))
        else:
            spread_word(range(2, len(reaches)))
        prepare(step)
        if step == 2:
            inner_rows = gathered(inner, sums)
            outer_parts = gathered_outer()
        if step == 2:
            break
        arrived(halo.at[1], bulk_r.at[1])
        arrived(e_halo.at[0, :, ends[1]], e_r.at[0])
        for side in range(2):
            seen = e_halo[0, side]
            ratio = seen / (0.5 + seen)
            base = LEFT if side == 0 else RIGHT
            for depth in range(2):
                factor(ratio, SUB - 1 - depth if side == 0 else depth, base + depth, base + depth)
        sums = fix(1, sums)

    odd = lax.rem(me, 2)

    def by_side(first, second):
        return [jnp.where(odd == 1, a, b) for a, b in zip(first, second)]

    def last_fix(side, start):
        arrived(halo.at[2, side], bulk_r.at[2 + side])
        arrived(e_halo.at[1, side, ends[1]], e_r.at[1 + side])
        slot, edge = LEFT + side * (RIGHT - LEFT), side * (SUB - 1)
        seen = e_halo[1, side, pl.ds((1 - side) * (SUB - 1), 1), :]
        ratio = jnp.broadcast_to(seen / (0.5 + seen), (SUB, 128))
        scale = [mask_b[slot] / (1.0 + freq[2, f] * ratio) for f in range(groups)]
        for f in range(groups):
            r_ref[slot + 4, f] = scale[f]

        def body(i, carry):
            total, acc = carry[0], carry[1:]
            d = side * quarter + i + (1 - side) * 2 * quarter * (i // quarter)
            moved, grown = [], []
            for f in range(groups):
                at = pl.ds((i * groups + f) * SUB, SUB)
                cell = (d * groups + f) * SUB + edge
                extra = r_ref[slot + 4, f] * (
                    halo[0, side, at, :] + coef[side, at, :] * halo[2, side, at, :])
                w_ref[cell] = w_ref[cell] + extra
                total = total + extra
                moved.append(extra)
                grown.append(g_ref[cell] * extra)
            return (total, *contribute(acc, d, moved, grown))

        return over_tiles(body, tuple(start), 6)

    west_edge = (sums[0], *outer_parts[0])
    east_edge = (sums[SUB - 1], *outer_parts[SUB - 1])
    near = last_fix(1 - odd, by_side(west_edge, east_edge))
    far = last_fix(odd, by_side(east_edge, west_edge))
    west_edge, east_edge = by_side(near, far), by_side(far, near)
    sums = (west_edge[0],) + tuple(sums[1:-1]) + (east_edge[0],)
    outer_parts = {0: west_edge[1:], SUB - 1: east_edge[1:]}

    last_factors(outer, sums)
    values = [None] * 8
    for j, x in enumerate(outer):
        part = outer_parts[x]
        values[j], values[2 + j] = part[0], part[1]
        for c in range(2):
            drift = zero
            for f in range(groups):
                drift = drift + (freq[3, f] * r_ref[x, f]) * part[2 + c * groups + f]
            values[4 + 2 * c + j] = drift
    all_rows = {**inner_rows, **row_sums(outer, values)}
    total = [all_rows[j] for j in range(4 * SUB)]
    pack, width = packing(n)
    if width > 4 * SUB:
        total.append(jnp.zeros((width - 4 * SUB, 128), jnp.float32))
    stacked = jnp.concatenate(total * pack, axis=0)
    picked = lax.dot_general(
        pick_t[...], stacked, (((1,), (1,)), ((), ())), precision=lax.Precision.HIGHEST,
        preferred_element_type=jnp.float32)
    row = lax.broadcasted_iota(jnp.int32, (SUB, 128), 0)
    mine = lax.rem(row, pack) == lane // width
    lines = 128 // n // pack
    for m in range(128 // SUB):
        tile = jnp.where(mine, picked[m * SUB:(m + 1) * SUB], 0.0)
        shift = 1
        while shift < pack:
            tile = tile + pltpu.roll(tile, SUB - shift, 0)
            shift *= 2
        for q in range(SUB // pack):
            k, line = divmod(m * (SUB // pack) + q, lines)
            sends[k, line:line + 1, :] = tile[q * pack:q * pack + 1]

    def begin(i, _):
        step = (i // 2) * (1 - 2 * lax.rem(i, 2))
        target = lax.rem(me + n // 2 + step + n, n)
        remote(sends.at[target], recv.at[me], a_s.at[0], a_r.at[0], target).start()
        return 0

    lax.fori_loop(1, n, begin, 0, unroll=3)
    recv[pl.ds(me, 1)] = sends[pl.ds(me, 1)]

    def write(d, _):
        for f in range(groups):
            for x in range(SUB):
                at = (d * groups + f) * SUB + x
                moved = w_ref[at]
                out[pl.ds((d * groups + f) * SUB * SUB + x, SUB, stride=SUB), :] = (
                    moved * g_ref[at] * r_ref[x, f])
        return 0

    lax.fori_loop(0, dirs, write, 0, unroll=2)
    arrived(send, bulk_s.at[0])
    arrived(wind_rows, small_s.at[0])
    arrived(land_rows, small_s.at[1])
    for s in range(2):
        arrived(e_halo.at[s, :, ends[1]], e_s.at[s])
    others = sends.at[pl.ds(0, n - 1)]
    arrived(others, a_s.at[0])
    arrived(others, a_r.at[0])


def finish_kernel(n, parts, out, recv, after, ocean_out, ocean, sem):
    rows = out.shape[0] // parts
    copies = []
    for q in range(parts):
        part = pl.ds(q * rows, rows)
        copies.append(pltpu.make_async_copy(out.at[part], after.at[part], sem.at[q]))
        copies[-1].start()
    band = 128 // n
    per_tile = 128 // SUB
    block = lax.broadcasted_iota(jnp.int32, (band, 128), 1) // SUB
    pack, width = packing(n)
    place = lax.rem(lax.broadcasted_iota(jnp.int32, (band, 128), 0), pack)
    unpacked = []
    for k in range(n):
        lines = recv[k]
        spread = jnp.concatenate(
            [jnp.broadcast_to(lines[q:q + 1], (pack, 128)) for q in range(band // pack)], axis=0)
        value = spread
        for j in range(1, pack):
            value = jnp.where(place == j, pltpu.roll(spread, 128 - j * width, 1), value)
        unpacked.append(value)
    for tile in range(max(1, n // per_tile)):
        for c in range(4):
            built = jnp.zeros((band, 128), jnp.float32)
            for k in range(min(n, per_tile)):
                moved = pltpu.roll(unpacked[tile * per_tile + k], (SUB * (k - c)) % 128, 1)
                built = jnp.where(block == k, moved, built)
            ocean[c, :, tile * 128:(tile + 1) * 128] = built
    copies.append(pltpu.make_async_copy(ocean, ocean_out, sem.at[parts]))
    copies[-1].start()
    for copy in copies:
        copy.wait()


def per_device(n, spectrum, wind, land_sea, band_rows):
    dirs, freqs, columns, lats = spectrum.shape
    groups = freqs // SUB
    half = dirs // 2 * groups * SUB
    band = lats // n
    f32 = jnp.float32
    anywhere = pl.BlockSpec(memory_space=pltpu.HBM)
    vmem = pl.BlockSpec(memory_space=pltpu.VMEM)
    cells = dirs * groups * SUB
    after, recv = pl.pallas_call(
        functools.partial(kernel, n, dirs, groups),
        out_shape=(pltpu.VMEM((cells * SUB, lats), f32), pltpu.VMEM((n, band // packing(n)[0], 128), f32)),
        in_specs=[anywhere] * 4,
        out_specs=(vmem, vmem),
        scratch_shapes=[
            pltpu.SMEM((2, dirs), f32),
            pltpu.VMEM((4, groups, SUB, lats), f32),
            pltpu.VMEM((2, SUB, lats), f32),
            pltpu.VMEM((SUB, lats), jnp.int32),
            pltpu.VMEM((1, lats), jnp.int32),
            pltpu.VMEM((cells, SUB, lats), f32),
            pltpu.VMEM((cells, SUB, lats), f32),
            pltpu.VMEM((cells, SUB, lats), f32),
            pltpu.VMEM((3, 2, half, lats), f32),
            pltpu.VMEM((3, 2, half, lats), f32),
            pltpu.VMEM((2, 2, SUB, lats), f32),
            pltpu.VMEM((2, SUB, lats), jnp.int32),
            pltpu.VMEM((2, 12, SUB, lats), f32),
            pltpu.VMEM((12, SUB, lats), f32),
            pltpu.VMEM((16, groups, SUB, lats), f32),
            pltpu.VMEM((SUB, groups, SUB, lats), f32),
            pltpu.VMEM((2, SUB, lats), f32),
            pltpu.VMEM((2, 2, SUB, lats), f32),
            pltpu.VMEM((128, 128), f32),
            pltpu.VMEM((n, band // packing(n)[0], 128), f32),
            pltpu.VMEM((2, half, lats), f32),
            pltpu.VMEM((3, dirs * groups, SUB, lats), f32),
            pltpu.VMEM((2, 2, half, lats), f32),
            pltpu.SemaphoreType.DMA((1,)),
            pltpu.SemaphoreType.DMA((3,)),
            pltpu.SemaphoreType.DMA((3,)),
            pltpu.SemaphoreType.REGULAR((max(1, (n // 2 - 1).bit_length()),)),
            pltpu.SemaphoreType.DMA((1,)),
            pltpu.SemaphoreType.DMA((4,)),
            pltpu.SemaphoreType.DMA((2,)),
            pltpu.SemaphoreType.DMA((2,)),
            pltpu.SemaphoreType.DMA((2,)),
            pltpu.SemaphoreType.DMA((3,)),
            pltpu.SemaphoreType.DMA((1,)),
            pltpu.SemaphoreType.DMA((1,)),
        ],
        compiler_params=pltpu.CompilerParams(
            collective_id=0, has_side_effects=True, vmem_limit_bytes=48 * 2**20),
        name="wave_window",
    )(*[pltpu.with_memory_space_constraint(a, pltpu.HBM) for a in (
        spectrum.reshape(cells, SUB, lats), wind, land_sea, band_rows.reshape(1, lats))])
    parts = 1
    after, ocean = pl.pallas_call(
        functools.partial(finish_kernel, n, parts),
        out_shape=(jax.ShapeDtypeStruct((cells * SUB, lats), f32),
                   jax.ShapeDtypeStruct((4, band, columns * n), f32)),
        in_specs=[vmem, vmem],
        out_specs=(anywhere, anywhere),
        scratch_shapes=[pltpu.VMEM((4, band, columns * n), f32), pltpu.SemaphoreType.DMA((parts + 1,))],
        compiler_params=pltpu.CompilerParams(vmem_limit_bytes=2**20),
        name="hand_over",
    )(after, recv)
    return after.reshape(spectrum.shape), ocean


def solution(mesh):
    placed = (
        P(None, None, ("member", "gx"), None),
        P(None, ("member", "gx"), None),
        P("gx", None),
        P(),
    )
    return jax.shard_map(
        functools.partial(per_device, mesh.shape["gx"]),
        mesh=mesh,
        in_specs=placed,
        out_specs=(P(None, None, ("member", "gx"), None), P(None, "gx", "member")),
        check_vma=False,
    )
```

```python
import functools
import math

import jax
import jax.numpy as jnp
from jax import lax
from jax.experimental import pallas as pl
from jax.experimental.pallas import tpu as pltpu
from jax.sharding import PartitionSpec as P

STEPS = 3
SUB = 8
LEFT, RIGHT = 8, 10


def packing(n):
    pack = min(4, 128 // n)
    return pack, 128 // pack


def kernel(n, dirs, groups, spec, wind_in, land_in, bands_in, out, recv,
           trig, freq, wind, land, bands, x_ref, w_ref, g_ref, send, halo, wind_h, land_h,
           wind_b, mask_b, r_ref, drift_ref, e_send, e_halo, pick_t, sends, coef, table, grow_h,
           in_sem, small_sem, col_sem, meet, bulk_s, bulk_r, small_s, small_r, e_s, e_r, a_s, a_r):
    me = lax.axis_index("gx")
    right, left = lax.rem(me + 1, n), lax.rem(me + n - 1, n)
    late = lax.rem((me + 1) // 2, 2) == 0

    def greet(semaphore, reach):
        for peer in (lax.rem(me + reach, n), lax.rem(me + n - reach, n)):
            pl.semaphore_signal(semaphore, inc=1, device_id={"gx": peer},
                                device_id_type=pl.DeviceIdType.MESH)

    barrier = pltpu.get_barrier_semaphore()
    greet(barrier, 1)
    reaches = [2 ** i for i in range((n // 2 - 1).bit_length())]
    quarter = dirs // 4
    qbins = quarter * groups * SUB
    cells = dirs * groups * SUB
    lane = lax.broadcasted_iota(jnp.int32, (SUB, 128), 1)
    x_rows = x_ref.reshape(cells * SUB, 128)

    in_copy = pltpu.make_async_copy(spec, x_ref, in_sem.at[0])

    def column_copies(k):
        return [pltpu.make_async_copy(
            spec.at[pl.ds(first, bins), column], send.at[k, side, pl.ds(to, bins)], col_sem.at[k])
            for first, bins, side, to, column in [
                (0, qbins, 0, 0, SUB - 1 - k), (3 * qbins, qbins, 0, qbins, SUB - 1 - k),
                (qbins, 2 * qbins, 1, 0, k)]]

    def columns_here(k):
        pltpu.make_async_copy(send.at[k], halo.at[k], col_sem.at[k]).wait()

    tables_in = [pltpu.make_async_copy(src, dst, small_sem.at[i]) for i, (src, dst) in enumerate(
        [(wind_in, wind), (land_in, land), (bands_in, bands)])]
    columns_in = [column_copies(k) for k in range(3)]
    for copy in columns_in[0] + tables_in:
        copy.start()
    in_copy.start()
    for copy in columns_in[1] + columns_in[2]:
        copy.start()

    for d in range(dirs):
        angle = (d + 0.5) * (2.0 * math.pi / dirs)
        trig[0, d] = jnp.float32(math.cos(angle))
        trig[1, d] = jnp.float32(math.sin(angle))
    freqs = groups * SUB
    for f in range(groups):
        level = (lax.broadcasted_iota(jnp.int32, (SUB, 128), 0) + f * SUB).astype(jnp.float32)
        weight = (level + 1.0) * (1.0 / freqs)
        grown = jnp.exp(level * math.log(1.1))
        freq[0, f] = 0.45 / grown
        freq[1, f] = grown * (2.0 * math.pi * 0.0418 / 9.81)
        freq[2, f] = 0.3 * weight * weight
        freq[3, f] = weight * (3.0 / math.sqrt(dirs * freqs))

    def remote(src, dst, send_sem, recv_sem, target):
        return pltpu.make_async_remote_copy(
            src_ref=src, dst_ref=dst, send_sem=send_sem, recv_sem=recv_sem,
            device_id={"gx": target}, device_id_type=pl.DeviceIdType.MESH)

    def arrived(ref, sem):
        pltpu.make_async_copy(ref, ref, sem).wait()

    bulk = [[remote(send.at[k, side], halo.at[k, side], bulk_s.at[0],
                    bulk_r.at[k + side * (k // 2)],
                    (right, left)[side]) for side in range(2)] for k in range(3)]
    ends = (pl.ds(SUB - 2, 2), pl.ds(0, 2))
    small = [remote(src, dst, small_s.at[j], small_r.at[j], (right, left)[side])
             for side in range(2) for j, (src, dst) in enumerate([
                 (wind.at[:, ends[side]], wind_h.at[side, :, ends[side]]),
                 (land.at[ends[side]], land_h.at[side, ends[side]])])]
    energy_msg = [[remote(e_send.at[s, ends[side]], e_halo.at[s, side, ends[side]], e_s.at[s],
                          e_r.at[s + side * s], (right, left)[side]) for side in range(2)] for s in range(2)]
    wind_rows, land_rows = wind_h.at[:, :, ends[1]], land_h.at[:, ends[1]]

    columns_here(0)
    pl.semaphore_wait(barrier, 2)
    for copy in tables_in:
        copy.wait()
    for copy in small + bulk[0]:
        copy.start()
    if reaches:
        greet(meet.at[0], reaches[0])

    def spread(slot, wind_tile, land_tile, column):
        for c in range(2):
            wind_b[c, slot] = jnp.broadcast_to(wind_tile[c][column:column + 1], (SUB, 128))
        mask_b[slot] = jnp.broadcast_to(
            land_tile[column:column + 1].astype(jnp.float32), (SUB, 128))

    own_wind = [wind[0], wind[1]]
    own_land = land[...]
    for x in range(SUB):
        spread(x, own_wind, own_land, x)

    columns_here(1)
    columns_here(2)

    def launch(k, when):
        @pl.when(when)
        def _():
            for copy in bulk[k]:
                copy.start()

    def spread_word(rounds):
        for i in rounds:
            pl.semaphore_wait(meet.at[i], 2)
            if i + 1 < len(reaches):
                greet(meet.at[i + 1], reaches[i + 1])

    inner_late = jnp.logical_and(late, jnp.logical_and(lax.rem(me, 2) == 1, me != n - 1))
    first_late = me == 0
    launch(1, jnp.logical_not(jnp.logical_or(inner_late, first_late)))
    in_copy.wait()

    def scalars(d):
        return trig[0, d], trig[1, d]

    halves = [(0, 2 * quarter, True), (quarter, 0, False)]

    def coefficients(cosine, sine, f, east, turn):
        k = freq[0, f]
        along_x = k * (cosine if east else -cosine)
        along_y = k * jnp.abs(sine)
        centre = 1.0 - along_x - along_y
        return centre, along_x, jnp.where(lane == 127 * turn, 0.0, along_y)

    def stencil(bin_tile):
        return table[0, bin_tile], table[1, bin_tile], table[2, bin_tile]

    def shifted(value, turn):
        return pltpu.roll(value, 1 + 126 * turn, 1)

    def growth_of(cosine, sine, f, slot):
        ratio = (wind_b[0, slot] * cosine + wind_b[1, slot] * sine) * freq[1, f]
        return 0.05 * jnp.minimum(jnp.maximum(ratio - 1.0, 0.0), 4.0)

    zero = jnp.zeros((SUB, 128), jnp.float32)

    def main(step, sums):
        for d0, skip, east in halves:
            def body(i, sums, d0=d0, skip=skip, east=east):
                turn = i // quarter
                d = d0 + i + skip * turn
                sums = list(sums)
                if step == 0:
                    cosine, sine = scalars(d)
                    speed = [wind_b[0, x] * cosine + wind_b[1, x] * sine for x in range(SUB)]
                for f in range(groups):
                    if step == 0:
                        centre, along_x, along_y = coefficients(cosine, sine, f, east, turn)
                        for c, value in enumerate((centre, along_x, along_y)):
                            table[c, d * groups + f] = value
                    else:
                        centre, along_x, along_y = stencil(d * groups + f)
                    before = None
                    for x in (range(SUB) if east else range(SUB - 1, -1, -1)):
                        at = (d * groups + f) * SUB + x
                        if step == 0:
                            value = x_rows[pl.ds((d * groups + f) * SUB * SUB + x, SUB, stride=SUB), :]
                            g_ref[at] = 1.0 + 0.05 * jnp.minimum(
                                jnp.maximum(speed[x] * freq[1, f] - 1.0, 0.0), 4.0)
                        else:
                            value = w_ref[at] * g_ref[at] * r_ref[x, f]
                        new = centre * value + along_y * shifted(value, turn)
                        if before is not None:
                            new = new + along_x * before
                        before = value
                        w_ref[at] = new
                        sums[x] = sums[x] + new
                return tuple(sums)

            sums = lax.fori_loop(0, 2 * quarter, body, tuple(sums), unroll=9)
        return sums

    def edges():
        for side, (d0, skip, east) in enumerate(halves):
            yield side, d0, skip, east, (LEFT if east else RIGHT), (0 if east else SUB - 1)

    def over_tiles(body, carry, unroll=3):
        return lax.fori_loop(0, 2 * quarter, body, carry, unroll=unroll)

    def grow_halo():
        for side, d0, skip, east, slot, edge in edges():
            def body(i, carry, d0=d0, skip=skip, side=side, slot=slot):
                d = d0 + i + skip * (i // quarter)
                cosine, sine = scalars(d)
                for f in range(groups):
                    for depth in range(2):
                        grow_h[side, depth, pl.ds((i * groups + f) * SUB, SUB), :] = (
                            1.0 + growth_of(cosine, sine, f, slot + depth))
                return carry

            over_tiles(body, 0)

    def prepare(step):
        for side, d0, skip, east, slot, edge in edges():
            def body(i, carry, d0=d0, skip=skip, east=east, side=side, slot=slot):
                turn = i // quarter
                d = d0 + i + skip * turn
                for f in range(groups):
                    centre, along_x, along_y = stencil(d * groups + f)
                    at = pl.ds((i * groups + f) * SUB, SUB)

                    def local(k, depth):
                        value = halo[k, side, at, :]
                        grown = grow_h[side, depth, at, :]
                        return (centre * value + along_y * shifted(value, turn)), grown

                    near, grown = local(0, 0)
                    if step == 1:
                        halo[0, side, at, :] = near * grown
                        coef[side, at, :] = along_x * grown
                    else:
                        far, grown_far = local(1, 1)
                        grown = along_x * grown
                        reach = along_x * grown_far * r_ref[slot + 1, f]
                        halo[0, side, at, :] = grown * (near + reach * far)
                        coef[side, at, :] = grown * reach * along_x
                return carry

            over_tiles(body, 0, 6)

    def contribute(acc, d, moved, grown):
        cosine, sine = scalars(d)
        acc = list(acc)
        flux = zero
        for f in range(groups):
            flux = flux + freq[3, f] * (grown[f] - moved[f])
            acc[2 + f] = acc[2 + f] + cosine * grown[f]
            acc[2 + groups + f] = acc[2 + groups + f] + sine * grown[f]
        acc[0] = acc[0] + cosine * flux
        acc[1] = acc[1] + sine * flux
        return acc

    def fix(step, sums):
        totals = {}
        for side, d0, skip, east, slot, edge in edges():
            def body(i, total, d0=d0, skip=skip, side=side, slot=slot, edge=edge):
                d = d0 + i + skip * (i // quarter)
                for f in range(groups):
                    at = pl.ds((i * groups + f) * SUB, SUB)
                    flow = halo[0, side, at, :]
                    if step == 1:
                        flow = r_ref[slot, f] * (flow + coef[side, at, :] * halo[1, side, at, :])
                        halo[0, side, at, :] = flow
                    extra = table[1, d * groups + f] * flow
                    cell = (d * groups + f) * SUB + edge
                    w_ref[cell] = w_ref[cell] + extra
                    total = total + extra
                return total

            totals[edge] = over_tiles(body, sums[edge], 6)
        return tuple(totals.get(x, sums[x]) for x in range(SUB))

    def energy_rows(sums, which):
        return [jnp.sum(sums[x] * mask_b[x], axis=0, keepdims=True) for x in which]

    def energy_tile(sums):
        return jnp.concatenate(energy_rows(sums, range(SUB)), axis=0) * (1.0 / cells)

    def factor(tile, column, mask_slot, slot):
        ratio = jnp.broadcast_to(tile[column:column + 1], (SUB, 128))
        for f in range(groups):
            r_ref[slot, f] = mask_b[mask_slot] / (1.0 + freq[2, f] * ratio)

    def own_factors(tile):
        ratio = tile / (0.5 + tile)
        for x in range(SUB):
            factor(ratio, x, x, x)

    inner, outer = list(range(1, SUB - 1)), [0, SUB - 1]

    def last_factors(which, sums):
        for x, row in zip(which, energy_rows(sums, which)):
            tile = row * (1.0 / cells)
            ratio = jnp.broadcast_to(tile / (0.5 + tile), (SUB, 128))
            for f in range(groups):
                r_ref[x, f] = mask_b[x] / (1.0 + freq[2, f] * ratio)

    def row_sums(which, values):
        rows_of = {}
        for c in range(4):
            for j, x in enumerate(which):
                value = values[c * len(which) + j]
                if c < 2:
                    value = value * mask_b[x]
                rows_of[c * SUB + x] = jnp.sum(value, axis=0, keepdims=True)
        return rows_of

    def gathered_outer():
        size = 2 + 2 * groups

        def gather(d, carry):
            done = []
            for j, x in enumerate(outer):
                cells_of = [(d * groups + f) * SUB + x for f in range(groups)]
                moved = [w_ref[at] for at in cells_of]
                grown = [g_ref[at] * value for at, value in zip(cells_of, moved)]
                done += contribute(carry[j * size:(j + 1) * size], d, moved, grown)
            return tuple(done)

        total = lax.fori_loop(0, dirs, gather, (zero,) * (2 * size), unroll=2)
        return {x: total[j * size:(j + 1) * size] for j, x in enumerate(outer)}

    def gathered(which, sums):
        last_factors(which, sums)
        for x in which:
            for f in range(groups):
                drift_ref[x, f] = freq[3, f] * r_ref[x, f]

        def gather(d, carry):
            cosine, sine = scalars(d)
            carry = list(carry)
            m = len(which)
            for j, x in enumerate(which):
                flux, drift = zero, zero
                for f in range(groups):
                    at = (d * groups + f) * SUB + x
                    moved = w_ref[at]
                    grown = g_ref[at] * moved
                    flux = flux + freq[3, f] * (grown - moved)
                    drift = drift + drift_ref[x, f] * grown
                carry[j] = carry[j] + cosine * flux
                carry[m + j] = carry[m + j] + sine * flux
                carry[2 * m + j] = carry[2 * m + j] + cosine * drift
                carry[3 * m + j] = carry[3 * m + j] + sine * drift
            return tuple(carry)

        return row_sums(which, lax.fori_loop(
            0, dirs, gather, (zero,) * (4 * len(which)), unroll=2))

    lat = lax.broadcasted_iota(jnp.int32, (128, 128), 0)
    pick_t[...] = (lat == bands[...]).astype(jnp.float32).T
    sums = main(0, (zero,) * SUB)
    spread_word(range(0, 1) if reaches else [])
    arrived(wind_rows, small_r.at[0])
    arrived(land_rows, small_r.at[1])
    for side in range(2):
        tiles = [wind_h[side, 0], wind_h[side, 1]]
        land_tile = land_h[side]
        for depth in range(2):
            spread((LEFT if side == 0 else RIGHT) + depth, tiles, land_tile,
                   SUB - 1 - depth if side == 0 else depth)
    grow_halo()
    arrived(halo.at[0], bulk_r.at[0])
    sums = fix(0, sums)
    for step in (1, 2):
        tile = energy_tile(sums)
        e_send[step - 1] = tile
        own_factors(tile)
        for copy in energy_msg[step - 1]:
            copy.start()
        if step == 1:
            launch(1, first_late)
        launch(2, late if step == 2 else jnp.logical_not(late))
        sums = main(step, (zero,) * SUB)
        if step == 1:
            launch(1, inner_late)
            spread_word(range(1, min(2, len(reaches))))
        else:
            spread_word(range(2, len(reaches)))
        prepare(step)
        if step == 1:
            pass
        if step == 2:
            inner_rows = gathered(inner, sums)
            outer_parts = gathered_outer()
        if step == 2:
            break
        arrived(halo.at[1], bulk_r.at[1])
        arrived(e_halo.at[0, :, ends[1]], e_r.at[0])
        for side in range(2):
            seen = e_halo[0, side]
            ratio = seen / (0.5 + seen)
            base = LEFT if side == 0 else RIGHT
            for depth in range(2):
                factor(ratio, SUB - 1 - depth if side == 0 else depth, base + depth, base + depth)
        sums = fix(1, sums)

    odd = lax.rem(me, 2)

    def by_side(first, second):
        return [jnp.where(odd == 1, a, b) for a, b in zip(first, second)]

    def last_fix(side, start):
        arrived(halo.at[2, side], bulk_r.at[2 + side])
        arrived(e_halo.at[1, side, ends[1]], e_r.at[1 + side])
        slot, edge = LEFT + side * (RIGHT - LEFT), side * (SUB - 1)
        seen = e_halo[1, side, pl.ds((1 - side) * (SUB - 1), 1), :]
        ratio = jnp.broadcast_to(seen / (0.5 + seen), (SUB, 128))
        scale = [mask_b[slot] / (1.0 + freq[2, f] * ratio) for f in range(groups)]
        for f in range(groups):
            r_ref[slot + 4, f] = scale[f]

        def body(i, carry):
            total, acc = carry[0], carry[1:]
            d = side * quarter + i + (1 - side) * 2 * quarter * (i // quarter)
            moved, grown = [], []
            for f in range(groups):
                at = pl.ds((i * groups + f) * SUB, SUB)
                cell = (d * groups + f) * SUB + edge
                extra = r_ref[slot + 4, f] * (
                    halo[0, side, at, :] + coef[side, at, :] * halo[2, side, at, :])
                w_ref[cell] = w_ref[cell] + extra
                total = total + extra
                moved.append(extra)
                grown.append(g_ref[cell] * extra)
            return (total, *contribute(acc, d, moved, grown))

        return over_tiles(body, tuple(start), 6)

    west_edge = (sums[0], *outer_parts[0])
    east_edge = (sums[SUB - 1], *outer_parts[SUB - 1])
    near = last_fix(1 - odd, by_side(west_edge, east_edge))
    far = last_fix(odd, by_side(east_edge, west_edge))
    west_edge, east_edge = by_side(near, far), by_side(far, near)
    sums = (west_edge[0],) + tuple(sums[1:-1]) + (east_edge[0],)
    outer_parts = {0: west_edge[1:], SUB - 1: east_edge[1:]}

    last_factors(outer, sums)
    values = [None] * 8
    for j, x in enumerate(outer):
        part = outer_parts[x]
        values[j], values[2 + j] = part[0], part[1]
        for c in range(2):
            drift = zero
            for f in range(groups):
                drift = drift + (freq[3, f] * r_ref[x, f]) * part[2 + c * groups + f]
            values[4 + 2 * c + j] = drift
    all_rows = {**inner_rows, **row_sums(outer, values)}
    total = [all_rows[j] for j in range(4 * SUB)]
    pack, width = packing(n)
    if width > 4 * SUB:
        total.append(jnp.zeros((width - 4 * SUB, 128), jnp.float32))
    stacked = jnp.concatenate(total * pack, axis=0)
    picked = lax.dot_general(
        pick_t[...], stacked, (((1,), (1,)), ((), ())), precision=lax.Precision.HIGHEST,
        preferred_element_type=jnp.float32)
    row = lax.broadcasted_iota(jnp.int32, (SUB, 128), 0)
    mine = lax.rem(row, pack) == lane // width
    lines = 128 // n // pack
    for m in range(128 // SUB):
        tile = jnp.where(mine, picked[m * SUB:(m + 1) * SUB], 0.0)
        shift = 1
        while shift < pack:
            tile = tile + pltpu.roll(tile, SUB - shift, 0)
            shift *= 2
        for q in range(SUB // pack):
            k, line = divmod(m * (SUB // pack) + q, lines)
            sends[k, line:line + 1, :] = tile[q * pack:q * pack + 1]

    def begin(i, _):
        step = (i // 2) * (1 - 2 * lax.rem(i, 2))
        target = lax.rem(me + n // 2 + step + n, n)
        remote(sends.at[target], recv.at[me], a_s.at[0], a_r.at[0], target).start()
        return 0

    lax.fori_loop(1, n, begin, 0, unroll=3)
    recv[pl.ds(me, 1)] = sends[pl.ds(me, 1)]

    def write(d, _):
        for f in range(groups):
            for x in range(SUB):
                at = (d * groups + f) * SUB + x
                moved = w_ref[at]
                out[pl.ds((d * groups + f) * SUB * SUB + x, SUB, stride=SUB), :] = (
                    moved * g_ref[at] * r_ref[x, f])
        return 0

    lax.fori_loop(0, dirs, write, 0, unroll=2)
    arrived(send, bulk_s.at[0])
    arrived(wind_rows, small_s.at[0])
    arrived(land_rows, small_s.at[1])
    for s in range(2):
        arrived(e_halo.at[s, :, ends[1]], e_s.at[s])
    others = sends.at[pl.ds(0, n - 1)]
    arrived(others, a_s.at[0])
    arrived(others, a_r.at[0])


def finish_kernel(n, parts, out, recv, after, ocean_out, ocean, sem):
    rows = out.shape[0] // parts
    copies = []
    for q in range(parts):
        part = pl.ds(q * rows, rows)
        copies.append(pltpu.make_async_copy(out.at[part], after.at[part], sem.at[q]))
        copies[-1].start()
    band = 128 // n
    per_tile = 128 // SUB
    block = lax.broadcasted_iota(jnp.int32, (band, 128), 1) // SUB
    pack, width = packing(n)
    place = lax.rem(lax.broadcasted_iota(jnp.int32, (band, 128), 0), pack)
    unpacked = []
    for k in range(n):
        lines = recv[k]
        spread = jnp.concatenate(
            [jnp.broadcast_to(lines[q:q + 1], (pack, 128)) for q in range(band // pack)], axis=0)
        value = spread
        for j in range(1, pack):
            value = jnp.where(place == j, pltpu.roll(spread, 128 - j * width, 1), value)
        unpacked.append(value)
    for tile in range(max(1, n // per_tile)):
        for c in range(4):
            built = jnp.zeros((band, 128), jnp.float32)
            for k in range(min(n, per_tile)):
                moved = pltpu.roll(unpacked[tile * per_tile + k], (SUB * (k - c)) % 128, 1)
                built = jnp.where(block == k, moved, built)
            ocean[c, :, tile * 128:(tile + 1) * 128] = built
    copies.append(pltpu.make_async_copy(ocean, ocean_out, sem.at[parts]))
    copies[-1].start()
    for copy in copies:
        copy.wait()


def per_device(n, spectrum, wind, land_sea, band_rows):
    dirs, freqs, columns, lats = spectrum.shape
    groups = freqs // SUB
    half = dirs // 2 * groups * SUB
    band = lats // n
    f32 = jnp.float32
    anywhere = pl.BlockSpec(memory_space=pltpu.HBM)
    vmem = pl.BlockSpec(memory_space=pltpu.VMEM)
    cells = dirs * groups * SUB
    after, recv = pl.pallas_call(
        functools.partial(kernel, n, dirs, groups),
        out_shape=(pltpu.VMEM((cells * SUB, lats), f32), pltpu.VMEM((n, band // packing(n)[0], 128), f32)),
        in_specs=[anywhere] * 4,
        out_specs=(vmem, vmem),
        scratch_shapes=[
            pltpu.SMEM((2, dirs), f32),
            pltpu.VMEM((4, groups, SUB, lats), f32),
            pltpu.VMEM((2, SUB, lats), f32),
            pltpu.VMEM((SUB, lats), jnp.int32),
            pltpu.VMEM((1, lats), jnp.int32),
            pltpu.VMEM((cells, SUB, lats), f32),
            pltpu.VMEM((cells, SUB, lats), f32),
            pltpu.VMEM((cells, SUB, lats), f32),
            pltpu.VMEM((3, 2, half, lats), f32),
            pltpu.VMEM((3, 2, half, lats), f32),
            pltpu.VMEM((2, 2, SUB, lats), f32),
            pltpu.VMEM((2, SUB, lats), jnp.int32),
            pltpu.VMEM((2, 12, SUB, lats), f32),
            pltpu.VMEM((12, SUB, lats), f32),
            pltpu.VMEM((16, groups, SUB, lats), f32),
            pltpu.VMEM((SUB, groups, SUB, lats), f32),
            pltpu.VMEM((2, SUB, lats), f32),
            pltpu.VMEM((2, 2, SUB, lats), f32),
            pltpu.VMEM((128, 128), f32),
            pltpu.VMEM((n, band // packing(n)[0], 128), f32),
            pltpu.VMEM((2, half, lats), f32),
            pltpu.VMEM((3, dirs * groups, SUB, lats), f32),
            pltpu.VMEM((2, 2, half, lats), f32),
            pltpu.SemaphoreType.DMA((1,)),
            pltpu.SemaphoreType.DMA((3,)),
            pltpu.SemaphoreType.DMA((3,)),
            pltpu.SemaphoreType.REGULAR((max(1, (n // 2 - 1).bit_length()),)),
            pltpu.SemaphoreType.DMA((1,)),
            pltpu.SemaphoreType.DMA((4,)),
            pltpu.SemaphoreType.DMA((2,)),
            pltpu.SemaphoreType.DMA((2,)),
            pltpu.SemaphoreType.DMA((2,)),
            pltpu.SemaphoreType.DMA((3,)),
            pltpu.SemaphoreType.DMA((1,)),
            pltpu.SemaphoreType.DMA((1,)),
        ],
        compiler_params=pltpu.CompilerParams(
            collective_id=0, has_side_effects=True, vmem_limit_bytes=48 * 2**20),
        name="wave_window",
    )(*[pltpu.with_memory_space_constraint(a, pltpu.HBM) for a in (
        spectrum.reshape(cells, SUB, lats), wind, land_sea, band_rows.reshape(1, lats))])
    parts = 1
    after, ocean = pl.pallas_call(
        functools.partial(finish_kernel, n, parts),
        out_shape=(jax.ShapeDtypeStruct((cells * SUB, lats), f32),
                   jax.ShapeDtypeStruct((4, band, columns * n), f32)),
        in_specs=[vmem, vmem],
        out_specs=(anywhere, anywhere),
        scratch_shapes=[pltpu.VMEM((4, band, columns * n), f32), pltpu.SemaphoreType.DMA((parts + 1,))],
        compiler_params=pltpu.CompilerParams(vmem_limit_bytes=2**20),
        name="hand_over",
    )(after, recv)
    return after.reshape(spectrum.shape), ocean


def solution(mesh):
    placed = (
        P(None, None, ("member", "gx"), None),
        P(None, ("member", "gx"), None),
        P("gx", None),
        P(),
    )
    return jax.shard_map(
        functools.partial(per_device, mesh.shape["gx"]),
        mesh=mesh,
        in_specs=placed,
        out_specs=(P(None, None, ("member", "gx"), None), P(None, "gx", "member")),
        check_vma=False,
    )
```

```python
import functools
import math

import jax
import jax.numpy as jnp
from jax import lax
from jax.experimental import pallas as pl
from jax.experimental.pallas import tpu as pltpu
from jax.sharding import PartitionSpec as P

STEPS = 3
SUB = 8
LEFT, RIGHT = 8, 10


def kernel(n, dirs, groups, spec, wind_in, land_in, bands_in, out, recv,
           trig, freq, wind, land, bands, x_ref, w_ref, g_ref, send, halo, wind_h, land_h,
           wind_b, mask_b, r_ref, drift_ref, e_send, e_halo, rows, sends, coef, table, grow_h,
           in_sem, small_sem, col_sem, meet, bulk_s, bulk_r, small_s, small_r, e_s, e_r, a_s, a_r):
    me = lax.axis_index("gx")
    right, left = lax.rem(me + 1, n), lax.rem(me + n - 1, n)
    late = lax.rem((me + 1) // 2, 2) == 0

    def greet(semaphore, reach):
        for peer in (lax.rem(me + reach, n), lax.rem(me + n - reach, n)):
            pl.semaphore_signal(semaphore, inc=1, device_id={"gx": peer},
                                device_id_type=pl.DeviceIdType.MESH)

    barrier = pltpu.get_barrier_semaphore()
    greet(barrier, 1)
    reaches = [2 ** i for i in range((n // 2 - 1).bit_length())]
    quarter = dirs // 4
    qbins = quarter * groups * SUB
    cells = dirs * groups * SUB
    lane = lax.broadcasted_iota(jnp.int32, (SUB, 128), 1)
    x_rows = x_ref.reshape(cells * SUB, 128)

    in_copy = pltpu.make_async_copy(spec, x_ref, in_sem.at[0])

    def column_copies(k):
        return [pltpu.make_async_copy(
            spec.at[pl.ds(first, bins), column], send.at[k, side, pl.ds(to, bins)], col_sem.at[k])
            for first, bins, side, to, column in [
                (0, qbins, 0, 0, SUB - 1 - k), (3 * qbins, qbins, 0, qbins, SUB - 1 - k),
                (qbins, 2 * qbins, 1, 0, k)]]

    def columns_here(k):
        pltpu.make_async_copy(send.at[k], halo.at[k], col_sem.at[k]).wait()

    tables_in = [pltpu.make_async_copy(src, dst, small_sem.at[i]) for i, (src, dst) in enumerate(
        [(wind_in, wind), (land_in, land), (bands_in, bands)])]
    columns_in = [column_copies(k) for k in range(3)]
    for copy in columns_in[0] + tables_in:
        copy.start()
    in_copy.start()
    for copy in columns_in[1] + columns_in[2]:
        copy.start()

    for d in range(dirs):
        angle = (d + 0.5) * (2.0 * math.pi / dirs)
        trig[0, d] = jnp.float32(math.cos(angle))
        trig[1, d] = jnp.float32(math.sin(angle))
    freqs = groups * SUB
    for f in range(groups):
        level = (lax.broadcasted_iota(jnp.int32, (SUB, 128), 0) + f * SUB).astype(jnp.float32)
        weight = (level + 1.0) * (1.0 / freqs)
        grown = jnp.exp(level * math.log(1.1))
        freq[0, f] = 0.45 / grown
        freq[1, f] = grown * (2.0 * math.pi * 0.0418 / 9.81)
        freq[2, f] = 0.3 * weight * weight
        freq[3, f] = weight * (3.0 / math.sqrt(dirs * freqs))

    def remote(src, dst, send_sem, recv_sem, target):
        return pltpu.make_async_remote_copy(
            src_ref=src, dst_ref=dst, send_sem=send_sem, recv_sem=recv_sem,
            device_id={"gx": target}, device_id_type=pl.DeviceIdType.MESH)

    def arrived(ref, sem):
        pltpu.make_async_copy(ref, ref, sem).wait()

    bulk = [[remote(send.at[k, side], halo.at[k, side], bulk_s.at[0], bulk_r.at[k],
                    (right, left)[side]) for side in range(2)] for k in range(3)]
    ends = (pl.ds(SUB - 2, 2), pl.ds(0, 2))
    small = [remote(src, dst, small_s.at[j], small_r.at[j], (right, left)[side])
             for side in range(2) for j, (src, dst) in enumerate([
                 (wind.at[:, ends[side]], wind_h.at[side, :, ends[side]]),
                 (land.at[ends[side]], land_h.at[side, ends[side]])])]
    energy_msg = [[remote(e_send.at[s, ends[side]], e_halo.at[s, side, ends[side]], e_s.at[s],
                          e_r.at[s], (right, left)[side]) for side in range(2)] for s in range(2)]
    wind_rows, land_rows = wind_h.at[:, :, ends[1]], land_h.at[:, ends[1]]

    columns_here(0)
    pl.semaphore_wait(barrier, 2)
    for copy in tables_in:
        copy.wait()
    for copy in small + bulk[0]:
        copy.start()
    if reaches:
        greet(meet.at[0], reaches[0])

    def spread(slot, wind_tile, land_tile, column):
        for c in range(2):
            wind_b[c, slot] = jnp.broadcast_to(wind_tile[c][column:column + 1], (SUB, 128))
        mask_b[slot] = jnp.broadcast_to(
            land_tile[column:column + 1].astype(jnp.float32), (SUB, 128))

    own_wind = [wind[0], wind[1]]
    own_land = land[...]
    for x in range(SUB):
        spread(x, own_wind, own_land, x)

    columns_here(1)
    columns_here(2)

    def launch(k, when):
        @pl.when(when)
        def _():
            for copy in bulk[k]:
                copy.start()

    def spread_word(rounds):
        for i in rounds:
            pl.semaphore_wait(meet.at[i], 2)
            if i + 1 < len(reaches):
                greet(meet.at[i + 1], reaches[i + 1])

    for copy in bulk[1]:
        copy.start()
    in_copy.wait()

    def scalars(d):
        return trig[0, d], trig[1, d]

    halves = [(0, 2 * quarter, True), (quarter, 0, False)]

    def coefficients(cosine, sine, f, east, turn):
        k = freq[0, f]
        along_x = k * (cosine if east else -cosine)
        along_y = k * jnp.abs(sine)
        centre = 1.0 - along_x - along_y
        return centre, along_x, jnp.where(lane == 127 * turn, 0.0, along_y)

    def stencil(bin_tile):
        return table[0, bin_tile], table[1, bin_tile], table[2, bin_tile]

    def shifted(value, turn):
        return pltpu.roll(value, 1 + 126 * turn, 1)

    def growth_of(cosine, sine, f, slot):
        ratio = (wind_b[0, slot] * cosine + wind_b[1, slot] * sine) * freq[1, f]
        return 0.05 * jnp.minimum(jnp.maximum(ratio - 1.0, 0.0), 4.0)

    zero = jnp.zeros((SUB, 128), jnp.float32)

    def main(step, sums):
        for d0, skip, east in halves:
            def body(i, sums, d0=d0, skip=skip, east=east):
                turn = i // quarter
                d = d0 + i + skip * turn
                sums = list(sums)
                if step == 0:
                    cosine, sine = scalars(d)
                    speed = [wind_b[0, x] * cosine + wind_b[1, x] * sine for x in range(SUB)]
                for f in range(groups):
                    if step == 0:
                        centre, along_x, along_y = coefficients(cosine, sine, f, east, turn)
                        for c, value in enumerate((centre, along_x, along_y)):
                            table[c, d * groups + f] = value
                    else:
                        centre, along_x, along_y = stencil(d * groups + f)
                    before = None
                    for x in (range(SUB) if east else range(SUB - 1, -1, -1)):
                        at = (d * groups + f) * SUB + x
                        if step == 0:
                            value = x_rows[pl.ds((d * groups + f) * SUB * SUB + x, SUB, stride=SUB), :]
                            g_ref[at] = 1.0 + 0.05 * jnp.minimum(
                                jnp.maximum(speed[x] * freq[1, f] - 1.0, 0.0), 4.0)
                        else:
                            value = w_ref[at] * g_ref[at] * r_ref[x, f]
                        new = centre * value + along_y * shifted(value, turn)
                        if before is not None:
                            new = new + along_x * before
                        before = value
                        w_ref[at] = new
                        sums[x] = sums[x] + new
                return tuple(sums)

            sums = lax.fori_loop(0, 2 * quarter, body, tuple(sums), unroll=9)
        return sums

    def edges():
        for side, (d0, skip, east) in enumerate(halves):
            yield side, d0, skip, east, (LEFT if east else RIGHT), (0 if east else SUB - 1)

    def over_tiles(body, carry, unroll=3):
        return lax.fori_loop(0, 2 * quarter, body, carry, unroll=unroll)

    def grow_halo():
        for side, d0, skip, east, slot, edge in edges():
            def body(i, carry, d0=d0, skip=skip, side=side, slot=slot):
                d = d0 + i + skip * (i // quarter)
                cosine, sine = scalars(d)
                for f in range(groups):
                    for depth in range(2):
                        grow_h[side, depth, pl.ds((i * groups + f) * SUB, SUB), :] = (
                            1.0 + growth_of(cosine, sine, f, slot + depth))
                return carry

            over_tiles(body, 0)

    def prepare(step):
        for side, d0, skip, east, slot, edge in edges():
            def body(i, carry, d0=d0, skip=skip, east=east, side=side, slot=slot):
                turn = i // quarter
                d = d0 + i + skip * turn
                for f in range(groups):
                    centre, along_x, along_y = stencil(d * groups + f)
                    at = pl.ds((i * groups + f) * SUB, SUB)

                    def local(k, depth):
                        value = halo[k, side, at, :]
                        grown = grow_h[side, depth, at, :]
                        return (centre * value + along_y * shifted(value, turn)), grown

                    near, grown = local(0, 0)
                    if step == 1:
                        halo[0, side, at, :] = near * grown
                        coef[side, at, :] = along_x * grown
                    else:
                        far, grown_far = local(1, 1)
                        grown = along_x * grown
                        reach = along_x * grown_far * r_ref[slot + 1, f]
                        halo[0, side, at, :] = grown * (near + reach * far)
                        coef[side, at, :] = grown * reach * along_x
                return carry

            over_tiles(body, 0, 6)

    def contribute(acc, d, moved, grown):
        cosine, sine = scalars(d)
        acc = list(acc)
        flux = zero
        for f in range(groups):
            flux = flux + freq[3, f] * (grown[f] - moved[f])
            acc[2 + f] = acc[2 + f] + cosine * grown[f]
            acc[2 + groups + f] = acc[2 + groups + f] + sine * grown[f]
        acc[0] = acc[0] + cosine * flux
        acc[1] = acc[1] + sine * flux
        return acc

    def fix(step, sums, parts=None):
        totals = {}
        for side, d0, skip, east, slot, edge in edges():
            def body(i, carry, d0=d0, skip=skip, side=side, slot=slot, edge=edge):
                total, acc = carry[0], carry[1:]
                d = d0 + i + skip * (i // quarter)
                moved, grown = [], []
                for f in range(groups):
                    at = pl.ds((i * groups + f) * SUB, SUB)
                    cell = (d * groups + f) * SUB + edge
                    if step == 0:
                        extra = table[1, d * groups + f] * halo[0, side, at, :]
                    else:
                        extra = r_ref[slot + 4 * (step - 1), f] * (
                            halo[0, side, at, :] + coef[side, at, :] * halo[step, side, at, :])
                        if step == 1:
                            halo[0, side, at, :] = extra
                            extra = table[1, d * groups + f] * extra
                    w_ref[cell] = w_ref[cell] + extra
                    total = total + extra
                    moved.append(extra)
                    if acc:
                        grown.append(g_ref[cell] * extra)
                if acc:
                    acc = contribute(acc, d, moved, grown)
                return (total, *acc)

            start = (sums[edge],) + (tuple(parts[edge]) if parts else ())
            done = over_tiles(body, start, 6)
            totals[edge] = done[0]
            if parts:
                parts[edge] = done[1:]
        return tuple(totals.get(x, sums[x]) for x in range(SUB))

    def energy_rows(sums, which):
        return [jnp.sum(sums[x] * mask_b[x], axis=0, keepdims=True) for x in which]

    def energy_tile(sums):
        return jnp.concatenate(energy_rows(sums, range(SUB)), axis=0) * (1.0 / cells)

    def factor(tile, column, mask_slot, slot):
        ratio = jnp.broadcast_to(tile[column:column + 1], (SUB, 128))
        for f in range(groups):
            r_ref[slot, f] = mask_b[mask_slot] / (1.0 + freq[2, f] * ratio)

    def own_factors(tile):
        ratio = tile / (0.5 + tile)
        for x in range(SUB):
            factor(ratio, x, x, x)

    inner, outer = list(range(1, SUB - 1)), [0, SUB - 1]

    def last_factors(which, sums):
        for x, row in zip(which, energy_rows(sums, which)):
            tile = row * (1.0 / cells)
            ratio = jnp.broadcast_to(tile / (0.5 + tile), (SUB, 128))
            for f in range(groups):
                r_ref[x, f] = mask_b[x] / (1.0 + freq[2, f] * ratio)

    def row_sums(which, values):
        rows_of = {}
        for c in range(4):
            for j, x in enumerate(which):
                value = values[c * len(which) + j]
                if c < 2:
                    value = value * mask_b[x]
                rows_of[c * SUB + x] = jnp.sum(value, axis=0, keepdims=True)
        return rows_of

    def gathered_outer():
        size = 2 + 2 * groups

        def gather(d, carry):
            done = []
            for j, x in enumerate(outer):
                cells_of = [(d * groups + f) * SUB + x for f in range(groups)]
                moved = [w_ref[at] for at in cells_of]
                grown = [g_ref[at] * value for at, value in zip(cells_of, moved)]
                done += contribute(carry[j * size:(j + 1) * size], d, moved, grown)
            return tuple(done)

        total = lax.fori_loop(0, dirs, gather, (zero,) * (2 * size), unroll=2)
        return {x: total[j * size:(j + 1) * size] for j, x in enumerate(outer)}

    def gathered(which, sums):
        last_factors(which, sums)
        for x in which:
            for f in range(groups):
                drift_ref[x, f] = freq[3, f] * r_ref[x, f]

        def gather(d, carry):
            cosine, sine = scalars(d)
            carry = list(carry)
            m = len(which)
            for j, x in enumerate(which):
                flux, drift = zero, zero
                for f in range(groups):
                    at = (d * groups + f) * SUB + x
                    moved = w_ref[at]
                    grown = g_ref[at] * moved
                    flux = flux + freq[3, f] * (grown - moved)
                    drift = drift + drift_ref[x, f] * grown
                carry[j] = carry[j] + cosine * flux
                carry[m + j] = carry[m + j] + sine * flux
                carry[2 * m + j] = carry[2 * m + j] + cosine * drift
                carry[3 * m + j] = carry[3 * m + j] + sine * drift
            return tuple(carry)

        return row_sums(which, lax.fori_loop(
            0, dirs, gather, (zero,) * (4 * len(which)), unroll=2))

    sums = main(0, (zero,) * SUB)
    spread_word(range(0, 1) if reaches else [])
    arrived(wind_rows, small_r.at[0])
    arrived(land_rows, small_r.at[1])
    for side in range(2):
        tiles = [wind_h[side, 0], wind_h[side, 1]]
        land_tile = land_h[side]
        for depth in range(2):
            spread((LEFT if side == 0 else RIGHT) + depth, tiles, land_tile,
                   SUB - 1 - depth if side == 0 else depth)
    grow_halo()
    arrived(halo.at[0], bulk_r.at[0])
    sums = fix(0, sums)
    outer_parts = None
    for step in (1, 2):
        tile = energy_tile(sums)
        e_send[step - 1] = tile
        own_factors(tile)
        for copy in energy_msg[step - 1]:
            copy.start()
        launch(2, late if step == 2 else jnp.logical_not(late))
        sums = main(step, (zero,) * SUB)
        if step == 1:
            spread_word(range(1, min(2, len(reaches))))
        else:
            spread_word(range(2, len(reaches)))
        prepare(step)
        if step == 2:
            inner_rows = gathered(inner, sums)
            outer_parts = gathered_outer()
        arrived(halo.at[step], bulk_r.at[step])
        arrived(e_halo.at[step - 1, :, ends[1]], e_r.at[step - 1])
        for side in range(2):
            seen = e_halo[step - 1, side]
            ratio = seen / (0.5 + seen)
            base = LEFT if side == 0 else RIGHT
            for depth in range(3 - step):
                factor(ratio, SUB - 1 - depth if side == 0 else depth, base + depth,
                       base + depth + 4 * (step - 1))
        sums = fix(step, sums, outer_parts)

    last_factors(outer, sums)
    values = [None] * 8
    for j, x in enumerate(outer):
        part = outer_parts[x]
        values[j], values[2 + j] = part[0], part[1]
        for c in range(2):
            drift = zero
            for f in range(groups):
                drift = drift + (freq[3, f] * r_ref[x, f]) * part[2 + c * groups + f]
            values[4 + 2 * c + j] = drift
    all_rows = {**inner_rows, **row_sums(outer, values)}
    total = [all_rows[j] for j in range(4 * SUB)]
    total.append(jnp.zeros((128 - 4 * SUB, 128), jnp.float32))
    stacked = jnp.concatenate(total, axis=0)
    lat = lax.broadcasted_iota(jnp.int32, (128, 128), 0)
    pick = (lat == bands[...]).astype(jnp.float32)
    picked = jnp.dot(stacked, pick, precision=lax.Precision.HIGHEST,
                     preferred_element_type=jnp.float32)
    rows[...] = picked.T
    band = 128 // n
    for k in range(n):
        sends[k] = rows[pl.ds(k * band, band), :]

    def begin(i, _):
        target = lax.rem(me + i, n)
        remote(sends.at[target], recv.at[me], a_s.at[0], a_r.at[0], target).start()
        return 0

    lax.fori_loop(1, n, begin, 0)
    recv[pl.ds(me, 1)] = sends[pl.ds(me, 1)]

    def write(d, _):
        for f in range(groups):
            for x in range(SUB):
                at = (d * groups + f) * SUB + x
                moved = w_ref[at]
                out[pl.ds((d * groups + f) * SUB * SUB + x, SUB, stride=SUB), :] = (
                    moved * g_ref[at] * r_ref[x, f])
        return 0

    lax.fori_loop(0, dirs, write, 0, unroll=2)
    arrived(send, bulk_s.at[0])
    arrived(wind_rows, small_s.at[0])
    arrived(land_rows, small_s.at[1])
    for s in range(2):
        arrived(e_halo.at[s, :, ends[1]], e_s.at[s])
    others = sends.at[pl.ds(0, n - 1)]
    arrived(others, a_s.at[0])
    arrived(others, a_r.at[0])


def finish_kernel(n, parts, out, recv, after, ocean_out, ocean, sem):
    rows = out.shape[0] // parts
    copies = []
    for q in range(parts):
        part = pl.ds(q * rows, rows)
        copies.append(pltpu.make_async_copy(out.at[part], after.at[part], sem.at[q]))
        copies[-1].start()
    band = 128 // n
    per_tile = 128 // SUB
    block = lax.broadcasted_iota(jnp.int32, (band, 128), 1) // SUB
    for tile in range(max(1, n // per_tile)):
        for c in range(4):
            built = jnp.zeros((band, 128), jnp.float32)
            for k in range(min(n, per_tile)):
                moved = pltpu.roll(recv[tile * per_tile + k], (SUB * (k - c)) % 128, 1)
                built = jnp.where(block == k, moved, built)
            ocean[c, :, tile * 128:(tile + 1) * 128] = built
    copies.append(pltpu.make_async_copy(ocean, ocean_out, sem.at[parts]))
    copies[-1].start()
    for copy in copies:
        copy.wait()


def per_device(n, spectrum, wind, land_sea, band_rows):
    dirs, freqs, columns, lats = spectrum.shape
    groups = freqs // SUB
    half = dirs // 2 * groups * SUB
    band = lats // n
    f32 = jnp.float32
    anywhere = pl.BlockSpec(memory_space=pltpu.HBM)
    vmem = pl.BlockSpec(memory_space=pltpu.VMEM)
    cells = dirs * groups * SUB
    after, recv = pl.pallas_call(
        functools.partial(kernel, n, dirs, groups),
        out_shape=(pltpu.VMEM((cells * SUB, lats), f32), pltpu.VMEM((n, band, 128), f32)),
        in_specs=[anywhere] * 4,
        out_specs=(vmem, vmem),
        scratch_shapes=[
            pltpu.SMEM((2, dirs), f32),
            pltpu.VMEM((4, groups, SUB, lats), f32),
            pltpu.VMEM((2, SUB, lats), f32),
            pltpu.VMEM((SUB, lats), jnp.int32),
            pltpu.VMEM((1, lats), jnp.int32),
            pltpu.VMEM((cells, SUB, lats), f32),
            pltpu.VMEM((cells, SUB, lats), f32),
            pltpu.VMEM((cells, SUB, lats), f32),
            pltpu.VMEM((3, 2, half, lats), f32),
            pltpu.VMEM((3, 2, half, lats), f32),
            pltpu.VMEM((2, 2, SUB, lats), f32),
            pltpu.VMEM((2, SUB, lats), jnp.int32),
            pltpu.VMEM((2, 12, SUB, lats), f32),
            pltpu.VMEM((12, SUB, lats), f32),
            pltpu.VMEM((16, groups, SUB, lats), f32),
            pltpu.VMEM((SUB, groups, SUB, lats), f32),
            pltpu.VMEM((2, SUB, lats), f32),
            pltpu.VMEM((2, 2, SUB, lats), f32),
            pltpu.VMEM((128, 128), f32),
            pltpu.VMEM((n, band, 128), f32),
            pltpu.VMEM((2, half, lats), f32),
            pltpu.VMEM((3, dirs * groups, SUB, lats), f32),
            pltpu.VMEM((2, 2, half, lats), f32),
            pltpu.SemaphoreType.DMA((1,)),
            pltpu.SemaphoreType.DMA((3,)),
            pltpu.SemaphoreType.DMA((3,)),
            pltpu.SemaphoreType.REGULAR((max(1, (n // 2 - 1).bit_length()),)),
            pltpu.SemaphoreType.DMA((1,)),
            pltpu.SemaphoreType.DMA((3,)),
            pltpu.SemaphoreType.DMA((2,)),
            pltpu.SemaphoreType.DMA((2,)),
            pltpu.SemaphoreType.DMA((2,)),
            pltpu.SemaphoreType.DMA((2,)),
            pltpu.SemaphoreType.DMA((1,)),
            pltpu.SemaphoreType.DMA((1,)),
        ],
        compiler_params=pltpu.CompilerParams(
            collective_id=0, has_side_effects=True, vmem_limit_bytes=48 * 2**20),
        name="wave_window",
    )(*[pltpu.with_memory_space_constraint(a, pltpu.HBM) for a in (
        spectrum.reshape(cells, SUB, lats), wind, land_sea, band_rows.reshape(1, lats))])
    parts = 1
    after, ocean = pl.pallas_call(
        functools.partial(finish_kernel, n, parts),
        out_shape=(jax.ShapeDtypeStruct((cells * SUB, lats), f32),
                   jax.ShapeDtypeStruct((4, band, columns * n), f32)),
        in_specs=[vmem, vmem],
        out_specs=(anywhere, anywhere),
        scratch_shapes=[pltpu.VMEM((4, band, columns * n), f32), pltpu.SemaphoreType.DMA((parts + 1,))],
        compiler_params=pltpu.CompilerParams(vmem_limit_bytes=2**20),
        name="hand_over",
    )(after, recv)
    return after.reshape(spectrum.shape), ocean


def solution(mesh):
    placed = (
        P(None, None, ("member", "gx"), None),
        P(None, ("member", "gx"), None),
        P("gx", None),
        P(),
    )
    return jax.shard_map(
        functools.partial(per_device, mesh.shape["gx"]),
        mesh=mesh,
        in_specs=placed,
        out_specs=(P(None, None, ("member", "gx"), None), P(None, "gx", "member")),
        check_vma=False,
    )
```
